32 devices in a mesh: blk: 8 (over y, x, core), row: 4 (over z).
Axes of the slice: x: 2, y: 2, z: 4, core: 2. Of those that a mesh axis runs over, the one named last changes fastest.
Arguments:
- rank_start: float32 [512, 128], P(('blk', 'row')), may hold values from 0.5 to 1.5
- tiles: bfloat16 [1024, 128, 128], P(('blk', 'row')), may hold values from 0 to 1
- tile_dest: int32 [1024], P(('blk', 'row')), may hold values from 0 to 63
- tile_src: int32 [1024], P(('blk', 'row')), may hold values from 0 to 127
- tile_fill: int32 [1024], P(('blk', 'row')), may hold values from 0 to 128
- out_degree: int32 [512, 128], P(('blk', 'row')), may hold values from 64 to 255
- dangling: int32 [512, 128], P(('blk', 'row')), may hold values 0 or 1
Outputs:
- rank: float32 [512, 128], P(('blk', 'row'))
- changes: float32 [2], replicated
The draws below stay inside these ranges and needn't reach their ends.
Inputs may be any that keep to these rules, and one draw needn't show every extreme that they name: `tile_fill`: 0 marks an empty slot.
All inputs are finite; a program needn't handle non-finite values. No bound on the sum of `dangling` on one device may be relied on, other than what follows from the above.
Results may differ from the reference program's by a relative error of at most 0.0003.
Values may be sent and summed in bfloat16 or wider, within the bound.
No kernel may reach another device: no remote copies, remote signals or barrier semaphores. Data moves between devices by JAX's collectives and lax.ppermute only.
A program may use at most 64 MiB of HBM per device.

```python
import jax
import jax.numpy as jnp
from jax import lax

TILE = 128
SH = 16
K = 32
ITERS = 2
PAGE_TILES = 512
SLOTS = 1024
N_BLK = 8
N_ROW = 4


def with_ends(drawn, key, low, top_value):
    place = [jax.random.randint(jax.random.fold_in(key, axis), (), 0, length) for axis, length in enumerate(drawn.shape)]
    widest = drawn.shape.index(max(drawn.shape))
    beside = place[:widest] + [(place[widest] + 1) % drawn.shape[widest]] + place[widest + 1:]
    return drawn.at[tuple(place)].set(low).at[tuple(beside)].set(top_value)


def block_scale(rng, extent, shards, low, top_value):
    def one(position, blocks):
        heights = jax.random.uniform(jax.random.fold_in(jax.random.fold_in(rng, 6), position), (blocks,), jnp.float32, low / len(shards), top_value / len(shards))
        return jnp.repeat(jnp.exp(heights), extent[position] // blocks).reshape((-1,) + (1,) * (len(extent) - position - 1))

    loudness = one(*shards[0])
    for cut in shards[1:]:
        loudness = loudness * one(*cut)
    return loudness


def setup_inputs(seed: int = 0) -> dict:
    arg_keys = jax.random.split(jax.random.key(seed), 8)
    return {
        "rank_start": jnp.clip(0.5 + 1.0 * jax.random.uniform(arg_keys[0], (PAGE_TILES, TILE), jnp.float32) ** block_scale(arg_keys[0], (PAGE_TILES, TILE), ((0, 32),), -0.2, 0.2), 0.5, 1.5),
        "tiles": jnp.clip(1.0 * jax.random.uniform(arg_keys[1], (SLOTS, TILE, TILE), jnp.float32) ** block_scale(arg_keys[1], (SLOTS, TILE, TILE), ((0, 32),), -0.2, 0.2), 0.0, 1.0).astype(jnp.bfloat16),
        "tile_dest": with_ends(jax.random.randint(arg_keys[2], (SLOTS,), 0, N_ROW * SH), jax.random.fold_in(arg_keys[2], 1), 0, (N_ROW * SH) - 1).astype(jnp.int32),
        "tile_src": with_ends(jax.random.randint(arg_keys[3], (SLOTS,), 0, N_BLK * SH), jax.random.fold_in(arg_keys[3], 1), 0, (N_BLK * SH) - 1).astype(jnp.int32),
        "tile_fill": with_ends(jax.random.randint(arg_keys[4], (SLOTS,), 0, 129), jax.random.fold_in(arg_keys[4], 1), 0, 128).astype(jnp.int32),
        "out_degree": with_ends(jax.random.randint(arg_keys[5], (PAGE_TILES, TILE), 32 * K // SH, 128 * K // SH), jax.random.fold_in(arg_keys[5], 1), 32 * K // SH, (128 * K // SH) - 1).astype(jnp.int32),
        "dangling": with_ends((jax.random.randint(arg_keys[6], (PAGE_TILES, TILE), 0, 8) < 1).astype(jnp.int32), jax.random.fold_in(arg_keys[6], 1), 0, 1),
    }


damping = 0.85


def reference(rank_start, tiles, tile_dest, tile_src, tile_fill, out_degree, dangling):
    groups = N_BLK * N_ROW
    tile_sets = tiles.reshape(groups, K, TILE, TILE)
    dest_sets = tile_dest.reshape(groups, K)
    source_sets = tile_src.reshape(groups, K)
    fill_sets = tile_fill.reshape(groups, K)
    dangle = dangling.astype(jnp.float32)
    weight = (1.0 - dangle) / out_degree.astype(jnp.float32)
    page_total = groups * SH * TILE
    lane_index = jnp.arange(TILE, dtype=jnp.int32)
    rank = rank_start
    change_list = []
    for iteration in range(ITERS):
        lost_mass = jnp.sum(rank * dangle)
        scaled = (rank * weight).astype(jnp.bfloat16)

        def one_group(incoming, index):
            block_index = index // N_ROW
            row_index = index % N_ROW
            source_ids = source_sets[index]
            global_src = ((source_ids // SH) * (N_ROW * SH) + row_index * SH + source_ids % SH).astype(jnp.int32)
            sources = scaled[global_src]
            column_mask = lane_index[None, :] < fill_sets[index][:, None]
            sources = jnp.where(column_mask, sources, jnp.zeros_like(sources))
            products = jnp.einsum("kij,kj->ki", tile_sets[index].astype(jnp.float32), sources.astype(jnp.float32))
            global_dest = (block_index * (N_ROW * SH) + dest_sets[index]).astype(jnp.int32)
            return incoming.at[global_dest].add(products), None

        incoming, unused = lax.scan(one_group, jnp.zeros(rank.shape, jnp.float32), jnp.arange(groups, dtype=jnp.int32))
        updated = damping * incoming + (1.0 - damping) + damping * lost_mass / page_total
        change_list.append(jnp.sum(jnp.abs(updated - rank)))
        rank = updated
    return rank, jnp.stack(change_list)
```

```python
import jax
import jax.numpy as jnp
from jax import lax
from jax.sharding import PartitionSpec as P

LANES = 128
SCALAR_ROWS = 8
damping = 0.85


def products_of(scaled, tiles, tile_dest, tile_src, column_mask, dest_tiles):
    select = (
        tile_src[:, None] == jnp.arange(scaled.shape[0], dtype=jnp.int32)[None, :]
    ).astype(jnp.bfloat16)
    picked = jnp.dot(select, scaled, preferred_element_type=jnp.float32)
    sources = picked.astype(jnp.bfloat16)
    sources = jnp.where(column_mask, sources, jnp.zeros_like(sources))
    products = jnp.einsum("kij,kj->ki", tiles, sources, preferred_element_type=jnp.float32)
    dest_select = (
        tile_dest[:, None] == jnp.arange(dest_tiles, dtype=jnp.int32)[None, :]
    ).astype(jnp.float32)
    return jnp.einsum("kd,ki->di", dest_select, products, precision=lax.Precision.HIGHEST)


def local(rank_start, tiles, tile_dest, tile_src, tile_fill, out_degree, dangling):
    share = rank_start.shape[0]
    blocks, rows = lax.axis_size("blk"), lax.axis_size("row")
    half = share // 2
    dest_tiles = rows * share
    page_total = blocks * rows * share * LANES
    b, w = lax.axis_index("blk"), lax.axis_index("row")
    core = b % 2
    column_mask = jnp.arange(LANES, dtype=jnp.int32)[None, :] < tile_fill[:, None]

    weight = (1.0 - dangling.astype(jnp.float32)) / out_degree.astype(jnp.float32)
    pack = jnp.concatenate([rank_start, weight], axis=0)
    got = lax.all_to_all(jnp.broadcast_to(pack[None], (blocks,) + pack.shape), "blk", 0, 0)
    rank0, weights = got[:, :share], got[:, share:]
    lost_here = jnp.where(weights == 0.0, 1.0, 0.0)

    scaled = (rank0 * weights).astype(jnp.bfloat16).reshape(blocks * share, LANES)
    lost0 = jnp.sum(rank0 * lost_here)
    part = products_of(scaled, tiles, tile_dest, tile_src, column_mask, dest_tiles)
    part = part + lost0 / page_total

    halves = part.reshape(rows, 2, half, LANES).transpose(1, 0, 2, 3)
    send = jnp.broadcast_to(halves[None], (blocks // 2,) + halves.shape)
    send = send.reshape(blocks * rows, half, LANES)
    got = lax.all_to_all(send, ("blk", "row"), 0, 0)
    mine = damping * jnp.sum(got.reshape(blocks, rows, half, LANES), axis=1) + (1.0 - damping)
    other = lax.ppermute(mine, "blk", [(i, i ^ 1) for i in range(blocks)])
    low = jnp.where(core == 0, mine, other)
    high = jnp.where(core == 0, other, mine)
    rank1 = jnp.concatenate([low, high], axis=1)

    change0 = jnp.sum(jnp.abs(rank1 - rank0))
    lost1 = jnp.sum(rank1 * lost_here)
    scaled = (rank1 * weights).astype(jnp.bfloat16).reshape(blocks * share, LANES)
    part = products_of(scaled, tiles, tile_dest, tile_src, column_mask, dest_tiles)
    part = damping * (part + lost1 / page_total)
    own = lax.dynamic_index_in_dim(rank1, b, 0, keepdims=False)
    is_own = (jnp.arange(rows) == w)[:, None, None]
    part = part.reshape(rows, share, LANES)
    less = jnp.where(is_own, part - (own - (1.0 - damping))[None], part)

    pack = jnp.concatenate(
        [less.reshape(dest_tiles, LANES), jnp.broadcast_to(change0, (SCALAR_ROWS, LANES))], axis=0
    )
    got = lax.all_to_all(jnp.broadcast_to(pack[None], (rows,) + pack.shape), "row", 0, 0)
    change1 = jnp.sum(jnp.abs(jnp.sum(got[:, :dest_tiles], axis=0)))
    change0 = jnp.sum(got[:, dest_tiles, 0])
    theirs = lax.dynamic_slice_in_dim(got, w * share, share, 1)
    own_part = lax.dynamic_index_in_dim(part, w, 0, keepdims=False)
    rank2 = jnp.sum(jnp.where(is_own, own_part[None], theirs), axis=0) + (1.0 - damping)

    got = lax.all_to_all(jnp.broadcast_to(change1, (blocks, 1, LANES)), "blk", 0, 0)
    change1 = jnp.sum(got[:, 0, 0])
    return rank2, jnp.stack([change0, change1])


def solution(mesh):
    placed = (
        P(("blk", "row"), None),
        P(("blk", "row"), None, None),
        P(("blk", "row")),
        P(("blk", "row")),
        P(("blk", "row")),
        P(("blk", "row"), None),
        P(("blk", "row"), None),
    )
    return jax.shard_map(
        local, mesh=mesh, in_specs=placed, out_specs=(P(("blk", "row"), None), P()), check_vma=False
    )
```

```python
import functools

import jax
import jax.numpy as jnp
from jax import lax
from jax.experimental import pallas as pl
from jax.experimental.pallas import tpu as pltpu
from jax.sharding import PartitionSpec as P

LANES = 128
SCALAR_ROWS = 8
damping = 0.85
VMEM = pl.BlockSpec(memory_space=pltpu.VMEM)
HBM = pl.BlockSpec(memory_space=pltpu.HBM)


def call(kernel, outs, scratch=(), space=VMEM):
    def run(*arguments):
        return pl.pallas_call(
            kernel,
            out_shape=outs,
            in_specs=(space,) * len(arguments),
            out_specs=(VMEM,) * len(outs) if isinstance(outs, tuple) else VMEM,
            scratch_shapes=scratch,
            compiler_params=pltpu.CompilerParams(vmem_limit_bytes=24 * 1024 * 1024),
            cost_estimate=pl.CostEstimate(flops=1000000, bytes_accessed=1000000, transcendentals=0),
        )(*arguments)

    return run


def column(row):
    n = row.shape[1]
    square = jnp.broadcast_to(row.astype(jnp.float32), (n, n))
    diagonal = lax.broadcasted_iota(jnp.int32, (n, n), 0) == lax.broadcasted_iota(jnp.int32, (n, n), 1)
    return jnp.sum(jnp.where(diagonal, square, 0.0), axis=1, keepdims=True)


def prepare(*refs):
    arguments, (payload, select, keep, dest_ids, tiles), scratch, sems = refs[:7], refs[7:12], refs[12:18], refs[18]
    copies = [
        pltpu.make_async_copy(source, target, sems.at[i])
        for i, (source, target) in enumerate(zip(arguments, (*scratch, tiles), strict=True))
    ]
    for copy in copies:
        copy.start()
    for copy in copies[:-1]:
        copy.wait()
    rank, degree, dangling, dest, src, fill = scratch
    share = rank.shape[0]
    weight = (1.0 - dangling[...].astype(jnp.float32)) / degree[...].astype(jnp.float32)
    payload[:, :share] = jnp.broadcast_to(rank[...][None], (payload.shape[0],) + rank.shape)
    payload[:, share:] = jnp.broadcast_to(weight[None], (payload.shape[0],) + rank.shape)
    lane = lax.broadcasted_iota(jnp.int32, select.shape, 1).astype(jnp.float32)
    select[...] = jnp.where(column(src[...]) == lane, 1.0, 0.0).astype(jnp.bfloat16)
    lane = lax.broadcasted_iota(jnp.int32, keep.shape, 1).astype(jnp.float32)
    keep[...] = jnp.where(lane < column(fill[...]), 1.0, 0.0)
    dest_ids[...] = jnp.broadcast_to(column(dest[...]), dest_ids.shape).astype(jnp.int32)
    copies[-1].wait()


def products(rank, weight, select, keep, dest_ids, tiles, sources, dest_tiles):
    scaled = (rank * weight).astype(jnp.bfloat16)
    picked = jnp.dot(select[...], scaled, preferred_element_type=jnp.float32)
    sources[...] = jnp.where(keep[...] > 0.0, picked, 0.0)
    target = lax.broadcasted_iota(jnp.int32, (dest_tiles, LANES), 0)
    total = jnp.zeros((dest_tiles, LANES), jnp.float32)
    for k in range(tiles.shape[0]):
        placed = jnp.where(dest_ids[pl.ds(k, 1), :] == target, sources[pl.ds(k, 1), :], 0.0)
        total += lax.dot_general(
            placed.astype(jnp.bfloat16),
            tiles[k],
            (((1,), (1,)), ((), ())),
            preferred_element_type=jnp.float32,
        )
    return total


def first(pages, rows, got, select, keep, dest_ids, tiles, send, sources):
    blocks, both, _ = got.shape
    share, half = both // 2, both // 4
    rank = got[:, :share].reshape(blocks * share, LANES)
    weight = got[:, share:].reshape(blocks * share, LANES)
    lost = jnp.sum(jnp.where(weight == 0.0, rank, 0.0))
    total = products(rank, weight, select, keep, dest_ids, tiles, sources, rows * share) + lost / pages
    for b in range(blocks):
        for w in range(rows):
            start = w * share + (b % 2) * half
            send[b * rows + w] = total[start : start + half]


def gather_rows(rows, got, mine):
    blocks = mine.shape[0]
    for b in range(blocks):
        total = got[b * rows]
        for w in range(1, rows):
            total += got[b * rows + w]
        mine[b] = damping * total + (1.0 - damping)


def second(pages, rows, mine, other, got, select, keep, dest_ids, tiles, send, own_part, sources):
    blocks, both, _ = got.shape
    share, half = both // 2, both // 4
    b, w = lax.axis_index("blk"), lax.axis_index("row")
    core0 = lax.rem(b, 2) == 0
    low = jnp.where(core0, mine[...], other[...])
    high = jnp.where(core0, other[...], mine[...])
    rank = jnp.concatenate([low, high], axis=1).reshape(blocks * share, LANES)
    rank0 = got[:, :share].reshape(blocks * share, LANES)
    weight = got[:, share:].reshape(blocks * share, LANES)
    change = jnp.sum(jnp.abs(rank - rank0))
    lost = jnp.sum(jnp.where(weight == 0.0, rank, 0.0))
    total = products(rank, weight, select, keep, dest_ids, tiles, sources, rows * share)
    total = damping * (total + lost / pages)
    own_low = jnp.where(core0, mine[b], other[b])
    own_high = jnp.where(core0, other[b], mine[b])
    own = jnp.concatenate([own_low, own_high], axis=0) - (1.0 - damping)
    kept = jnp.zeros((share, LANES), jnp.float32)
    for r in range(rows):
        piece = total[r * share : (r + 1) * share]
        kept = jnp.where(w == r, piece, kept)
        less = jnp.where(w == r, piece - own, piece)
        for to in range(rows):
            send[to, r * share : (r + 1) * share] = less
    own_part[...] = kept
    for to in range(rows):
        send[to, rows * share :] = jnp.full((SCALAR_ROWS, LANES), change, jnp.float32)


def block_change(got, send):
    rows, height, _ = got.shape
    dest_tiles = height - SCALAR_ROWS
    total = got[0]
    for r in range(1, rows):
        total += got[r]
    change1 = jnp.sum(jnp.abs(total[:dest_tiles]))
    change0 = jnp.where(lax.axis_index("blk") == 0, total[dest_tiles:, :], 0.0)[:1]
    lane = lax.broadcasted_iota(jnp.int32, (1, LANES), 1)
    line = jnp.where(lane == 0, change0, change1)
    send[...] = jnp.broadcast_to(line, send.shape)


def finish(rows, got, own_part, changes, rank, out):
    share = rank.shape[0]
    w = lax.axis_index("row")
    total = own_part[...] + (1.0 - damping)
    for r in range(rows):
        total += jnp.where(w == r, 0.0, got[r, pl.ds(w * share, share), :])
    rank[...] = total
    out[...] = jnp.sum(changes[...], axis=0)[: out.shape[0]]


def local(rank_start, tiles, tile_dest, tile_src, tile_fill, out_degree, dangling):
    share, slots = rank_start.shape[0], tiles.shape[0]
    blocks, rows = lax.axis_size("blk"), lax.axis_size("row")
    half, dest_tiles = share // 2, rows * share
    pages = float(blocks * rows * share * LANES)
    f32 = functools.partial(jax.ShapeDtypeStruct, dtype=jnp.float32)
    sources = (pltpu.VMEM((slots, LANES), jnp.float32),)

    arguments = (rank_start, out_degree, dangling, tile_dest[None], tile_src[None], tile_fill[None], tiles)
    payload, *table = call(
        prepare,
        (
            f32((blocks, 2 * share, LANES)),
            jax.ShapeDtypeStruct((slots, blocks * share), jnp.bfloat16),
            f32((slots, LANES)),
            jax.ShapeDtypeStruct((slots, LANES), jnp.int32),
            jax.ShapeDtypeStruct(tiles.shape, tiles.dtype),
        ),
        (*(pltpu.VMEM(a.shape, a.dtype) for a in arguments[:-1]), pltpu.SemaphoreType.DMA((len(arguments),))),
        HBM,
    )(*(pltpu.with_memory_space_constraint(a, pltpu.HBM) for a in arguments))

    got_a = lax.all_to_all(payload, "blk", 0, 0)
    send = call(functools.partial(first, pages, rows), f32((blocks * rows, half, LANES)), sources)(got_a, *table)

    got_b = lax.all_to_all(send, ("blk", "row"), 0, 0)
    mine = call(functools.partial(gather_rows, rows), f32((blocks, half, LANES)))(got_b)
    other = lax.ppermute(mine, "blk", [(i, i ^ 1) for i in range(blocks)])
    send, own_part = call(
        functools.partial(second, pages, rows),
        (f32((rows, dest_tiles + SCALAR_ROWS, LANES)), f32((share, LANES))),
        sources,
    )(mine, other, got_a, *table)

    got_d = lax.all_to_all(send, "row", 0, 0)
    send = call(block_change, f32((blocks, LANES)))(got_d)

    got_e = lax.all_to_all(send, "blk", 0, 0, tiled=True)
    return call(functools.partial(finish, rows), (f32((share, LANES)), f32((2,))))(got_d, own_part, got_e)


def solution(mesh):
    placed = (
        P(("blk", "row"), None),
        P(("blk", "row"), None, None),
        P(("blk", "row")),
        P(("blk", "row")),
        P(("blk", "row")),
        P(("blk", "row"), None),
        P(("blk", "row"), None),
    )
    return jax.shard_map(
        local, mesh=mesh, in_specs=placed, out_specs=(P(("blk", "row"), None), P()), check_vma=False
    )
```

```python
import functools

import jax
import jax.numpy as jnp
from jax import lax
from jax.experimental import pallas as pl
from jax.experimental.pallas import tpu as pltpu
from jax.sharding import PartitionSpec as P

LANES = 128
SCALAR_ROWS = 8
FLAG = 32.0
damping = 0.85
VMEM = pl.BlockSpec(memory_space=pltpu.VMEM)
HBM = pl.BlockSpec(memory_space=pltpu.HBM)


def call(kernel, outs, scratch=(), space=VMEM):
    def run(*arguments):
        return pl.pallas_call(
            kernel,
            out_shape=outs,
            in_specs=(space,) * len(arguments),
            out_specs=(VMEM,) * len(outs) if isinstance(outs, tuple) else VMEM,
            scratch_shapes=scratch,
            compiler_params=pltpu.CompilerParams(vmem_limit_bytes=24 * 1024 * 1024),
            cost_estimate=pl.CostEstimate(flops=1000000, bytes_accessed=1000000, transcendentals=0),
        )(*arguments)

    return run


def column(row):
    n = row.shape[1]
    square = jnp.broadcast_to(row.astype(jnp.float32), (n, n))
    diagonal = lax.broadcasted_iota(jnp.int32, (n, n), 0) == lax.broadcasted_iota(jnp.int32, (n, n), 1)
    return jnp.sum(jnp.where(diagonal, square, 0.0), axis=1, keepdims=True)


def prepare(*refs):
    arguments, (payload, select, keep, dest_ids, tiles, start), scratch, sems = refs[:7], refs[7:13], refs[13:19], refs[19]
    copies = [
        pltpu.make_async_copy(source, target, sems.at[i])
        for i, (source, target) in enumerate(zip(arguments, (*scratch, tiles), strict=True))
    ]
    for copy in copies:
        copy.start()
    for copy in copies[:-1]:
        copy.wait()
    rank, degree, dangling, dest, src, fill = scratch
    share = rank.shape[0]
    stuck = dangling[...] > 0
    degree, rank = degree[...].astype(jnp.float32), rank[...]
    scaled = (rank * (1.0 / degree)).astype(jnp.bfloat16).astype(jnp.float32)
    high = rank.astype(jnp.bfloat16).astype(jnp.float32)
    planes = [jnp.where(stuck, high, scaled), jnp.where(stuck, rank - high, degree)]
    for i, plane in enumerate(planes):
        rows = slice(i * share, (i + 1) * share)
        payload[:, rows] = jnp.broadcast_to(plane.astype(jnp.bfloat16)[None], (payload.shape[0], share, LANES))
    start[...] = rank
    lane = lax.broadcasted_iota(jnp.int32, select.shape, 1).astype(jnp.float32)
    select[...] = jnp.where(column(src[...]) == lane, 1.0, 0.0).astype(jnp.bfloat16)
    lane = lax.broadcasted_iota(jnp.int32, keep.shape, 1).astype(jnp.float32)
    keep[...] = jnp.where(lane < column(fill[...]), 1.0, 0.0)
    dest_ids[...] = jnp.broadcast_to(column(dest[...]), dest_ids.shape).astype(jnp.int32)
    copies[-1].wait()


def unpack(got):
    blocks, both, _ = got.shape
    one = got[:, : both // 2].reshape(blocks * both // 2, LANES).astype(jnp.float32)
    two = got[:, both // 2 :].reshape(blocks * both // 2, LANES).astype(jnp.float32)
    return one, two, two < FLAG


def products(scaled, select, keep, dest_ids, tiles, sources, dest_tiles):
    picked = jnp.dot(select[...], scaled.astype(jnp.bfloat16), preferred_element_type=jnp.float32)
    sources[...] = jnp.where(keep[...] > 0.0, picked, 0.0)
    target = lax.broadcasted_iota(jnp.int32, (dest_tiles, LANES), 0)
    total = jnp.zeros((dest_tiles, LANES), jnp.float32)
    slots = tiles.shape[0]
    together = 2 - slots % 2

    def placed(k):
        line = jnp.where(dest_ids[pl.ds(k, 1), :] == target, sources[pl.ds(k, 1), :], 0.0)
        return line.astype(jnp.bfloat16)

    for first_slot in range(0, slots, together):
        group = range(first_slot, first_slot + together)
        total += lax.dot_general(
            jnp.concatenate([placed(k) for k in group], axis=1),
            jnp.concatenate([tiles[k] for k in group], axis=1),
            (((1,), (1,)), ((), ())),
            preferred_element_type=jnp.float32,
        )
    return total


def first(pages, rows, got, select, keep, dest_ids, tiles, send, sources):
    blocks, both, _ = got.shape
    share, half = both // 2, both // 4
    one, two, stuck = unpack(got)
    lost = jnp.sum(jnp.where(stuck, one + two, 0.0))
    scaled = jnp.where(stuck, 0.0, one)
    total = products(scaled, select, keep, dest_ids, tiles, sources, rows * share) + lost / pages
    for b in range(blocks):
        for w in range(rows):
            start = w * share + (b % 2) * half
            send[b * rows + w] = total[start : start + half]


def gather_rows(rows, got, mine):
    blocks = mine.shape[0]
    for b in range(blocks):
        total = got[b * rows]
        for w in range(1, rows):
            total += got[b * rows + w]
        mine[b] = damping * total + (1.0 - damping)


def second(pages, rows, mine, other, got, start, select, keep, dest_ids, tiles, send, own_part, sources):
    blocks, both, _ = got.shape
    share, half = both // 2, both // 4
    b, w = lax.axis_index("blk"), lax.axis_index("row")
    core0 = lax.rem(b, 2) == 0
    low = jnp.where(core0, mine[...], other[...])
    high = jnp.where(core0, other[...], mine[...])
    rank = jnp.concatenate([low, high], axis=1).reshape(blocks * share, LANES)
    _, degree, stuck = unpack(got)
    lost = jnp.sum(jnp.where(stuck, rank, 0.0))
    scaled = rank * jnp.where(stuck, 0.0, 1.0 / degree)
    total = products(scaled, select, keep, dest_ids, tiles, sources, rows * share)
    total = damping * (total + lost / pages)
    own_low = jnp.where(core0, mine[b], other[b])
    own_high = jnp.where(core0, other[b], mine[b])
    own = jnp.concatenate([own_low, own_high], axis=0)
    change = jnp.sum(jnp.abs(own - start[...]))
    own -= 1.0 - damping
    kept = jnp.zeros((share, LANES), jnp.float32)
    for r in range(rows):
        piece = total[r * share : (r + 1) * share]
        kept = jnp.where(w == r, piece, kept)
        less = jnp.where(w == r, piece - own, piece)
        for to in range(rows):
            send[to, r * share : (r + 1) * share] = less
    own_part[...] = kept
    for to in range(rows):
        send[to, rows * share :] = jnp.full((SCALAR_ROWS, LANES), change, jnp.float32)


def block_change(got, send):
    rows, height, _ = got.shape
    dest_tiles = height - SCALAR_ROWS
    total = got[0]
    for r in range(1, rows):
        total += got[r]
    change1 = jnp.sum(jnp.abs(total[:dest_tiles]))
    lane = lax.broadcasted_iota(jnp.int32, (1, LANES), 1)
    line = jnp.where(lane == 0, total[dest_tiles : dest_tiles + 1], change1)
    send[...] = jnp.broadcast_to(line, send.shape)


def finish(rows, got, own_part, changes, rank, out):
    share = rank.shape[0]
    w = lax.axis_index("row")
    total = own_part[...] + (1.0 - damping)
    for r in range(rows):
        total += jnp.where(w == r, 0.0, got[r, pl.ds(w * share, share), :])
    rank[...] = total
    out[...] = jnp.sum(changes[...], axis=0)[: out.shape[0]]


def local(rank_start, tiles, tile_dest, tile_src, tile_fill, out_degree, dangling):
    share, slots = rank_start.shape[0], tiles.shape[0]
    blocks, rows = lax.axis_size("blk"), lax.axis_size("row")
    half, dest_tiles = share // 2, rows * share
    pages = float(blocks * rows * share * LANES)
    f32 = functools.partial(jax.ShapeDtypeStruct, dtype=jnp.float32)
    sources = (pltpu.VMEM((slots, LANES), jnp.float32),)

    arguments = (rank_start, out_degree, dangling, tile_dest[None], tile_src[None], tile_fill[None], tiles)
    payload, *table, start = call(
        prepare,
        (
            jax.ShapeDtypeStruct((blocks, 2 * share, LANES), jnp.bfloat16),
            jax.ShapeDtypeStruct((slots, blocks * share), jnp.bfloat16),
            f32((slots, LANES)),
            jax.ShapeDtypeStruct((slots, LANES), jnp.int32),
            jax.ShapeDtypeStruct(tiles.shape, tiles.dtype),
            f32((share, LANES)),
        ),
        (*(pltpu.VMEM(a.shape, a.dtype) for a in arguments[:-1]), pltpu.SemaphoreType.DMA((len(arguments),))),
        HBM,
    )(*(pltpu.with_memory_space_constraint(a, pltpu.HBM) for a in arguments))

    got_a = lax.all_to_all(payload, "blk", 0, 0)
    send = call(functools.partial(first, pages, rows), f32((blocks * rows, half, LANES)), sources)(got_a, *table)

    got_b = lax.all_to_all(send, ("blk", "row"), 0, 0)
    mine = call(functools.partial(gather_rows, rows), f32((blocks, half, LANES)))(got_b)
    other = lax.ppermute(mine, "blk", [(i, i ^ 1) for i in range(blocks)])
    send, own_part = call(
        functools.partial(second, pages, rows),
        (f32((rows, dest_tiles + SCALAR_ROWS, LANES)), f32((share, LANES))),
        sources,
    )(mine, other, got_a, start, *table)

    got_d = lax.all_to_all(send, "row", 0, 0)
    send = call(block_change, f32((blocks, LANES)))(got_d)

    got_e = lax.all_to_all(send, "blk", 0, 0, tiled=True)
    return call(functools.partial(finish, rows), (f32((share, LANES)), f32((2,))))(got_d, own_part, got_e)


def solution(mesh):
    placed = (
        P(("blk", "row"), None),
        P(("blk", "row"), None, None),
        P(("blk", "row")),
        P(("blk", "row")),
        P(("blk", "row")),
        P(("blk", "row"), None),
        P(("blk", "row"), None),
    )
    return jax.shard_map(
        local, mesh=mesh, in_specs=placed, out_specs=(P(("blk", "row"), None), P()), check_vma=False
    )
```

```python
import functools

import jax
import jax.numpy as jnp
from jax import lax
from jax.experimental import pallas as pl
from jax.experimental.pallas import tpu as pltpu
from jax.sharding import PartitionSpec as P

LANES = 128
SCALAR_ROWS = 8
FLAG = 32.0
damping = 0.85
VMEM = pl.BlockSpec(memory_space=pltpu.VMEM)
HBM = pl.BlockSpec(memory_space=pltpu.HBM)


def call(kernel, outs, scratch=(), space=VMEM, flops=1000000):
    def run(*arguments):
        return pl.pallas_call(
            kernel,
            out_shape=outs,
            in_specs=(space,) * len(arguments),
            out_specs=(VMEM,) * len(outs) if isinstance(outs, tuple) else VMEM,
            scratch_shapes=scratch,
            compiler_params=pltpu.CompilerParams(vmem_limit_bytes=24 * 1024 * 1024),
            cost_estimate=pl.CostEstimate(flops=flops, bytes_accessed=1000000, transcendentals=0),
        )(*arguments)

    return run


def column(row):
    n = row.shape[1]
    square = jnp.broadcast_to(row.astype(jnp.float32), (n, n))
    diagonal = lax.broadcasted_iota(jnp.int32, (n, n), 0) == lax.broadcasted_iota(jnp.int32, (n, n), 1)
    return jnp.sum(jnp.where(diagonal, square, 0.0), axis=1, keepdims=True)


def prepare(*refs):
    arguments, (payload, select, keep, dest_ids, start), scratch, sems = refs[:6], refs[6:11], refs[11:17], refs[17]
    copies = [
        pltpu.make_async_copy(source, target, sems.at[i])
        for i, (source, target) in enumerate(zip(arguments, scratch, strict=True))
    ]
    for copy in copies:
        copy.start()
    for copy in copies:
        copy.wait()
    rank, degree, dangling, dest, src, fill = scratch
    share = rank.shape[0]
    stuck = dangling[...] > 0
    degree, rank = degree[...].astype(jnp.float32), rank[...]
    scaled = (rank * (1.0 / degree)).astype(jnp.bfloat16).astype(jnp.float32)
    high = rank.astype(jnp.bfloat16).astype(jnp.float32)
    planes = [jnp.where(stuck, high, scaled), jnp.where(stuck, rank - high, degree)]
    for i, plane in enumerate(planes):
        rows = slice(i * share, (i + 1) * share)
        payload[:, rows] = jnp.broadcast_to(plane.astype(jnp.bfloat16)[None], (payload.shape[0], share, LANES))
    start[...] = rank
    lane = lax.broadcasted_iota(jnp.int32, select.shape, 1).astype(jnp.float32)
    select[...] = jnp.where(column(src[...]) == lane, 1.0, 0.0).astype(jnp.bfloat16)
    lane = lax.broadcasted_iota(jnp.int32, keep.shape, 1).astype(jnp.float32)
    keep[...] = jnp.where(lane < column(fill[...]), 1.0, 0.0)
    dest_ids[...] = jnp.broadcast_to(column(dest[...]), dest_ids.shape).astype(jnp.int32)


def unpack(got):
    blocks, both, _ = got.shape
    one = got[:, : both // 2].reshape(blocks * both // 2, LANES).astype(jnp.float32)
    two = got[:, both // 2 :].reshape(blocks * both // 2, LANES).astype(jnp.float32)
    return one, two, two < FLAG


def products(scaled, select, keep, dest_ids, tiles, sources, dest_tiles):
    picked = jnp.dot(select[...], scaled.astype(jnp.bfloat16), preferred_element_type=jnp.float32)
    sources[...] = jnp.where(keep[...] > 0.0, picked, 0.0)
    target = lax.broadcasted_iota(jnp.int32, (dest_tiles, LANES), 0)
    total = jnp.zeros((dest_tiles, LANES), jnp.float32)
    slots = tiles.shape[0]
    together = 2 - slots % 2

    def placed(k):
        line = jnp.where(dest_ids[pl.ds(k, 1), :] == target, sources[pl.ds(k, 1), :], 0.0)
        return line.astype(jnp.bfloat16)

    for first_slot in range(0, slots, together):
        group = range(first_slot, first_slot + together)
        total += lax.dot_general(
            jnp.concatenate([placed(k) for k in group], axis=1),
            jnp.concatenate([tiles[k] for k in group], axis=1),
            (((1,), (1,)), ((), ())),
            preferred_element_type=jnp.float32,
        )
    return total


def first(pages, rows, got, select, keep, dest_ids, tiles, send, sources):
    blocks, both, _ = got.shape
    share, half = both // 2, both // 4
    one, two, stuck = unpack(got)
    lost = jnp.sum(jnp.where(stuck, one + two, 0.0))
    scaled = jnp.where(stuck, 0.0, one)
    total = products(scaled, select, keep, dest_ids, tiles, sources, rows * share) + lost / pages
    for b in range(blocks):
        for w in range(rows):
            start = w * share + (b % 2) * half
            send[b * rows + w] = total[start : start + half]


def gather_rows(rows, got, mine):
    blocks = mine.shape[0]
    for b in range(blocks):
        total = got[b * rows]
        for w in range(1, rows):
            total += got[b * rows + w]
        mine[b] = damping * total + (1.0 - damping)


def second(pages, rows, mine, other, got, start, select, keep, dest_ids, tiles, send, own_part, sources):
    blocks, both, _ = got.shape
    share, half = both // 2, both // 4
    b, w = lax.axis_index("blk"), lax.axis_index("row")
    core0 = lax.rem(b, 2) == 0
    low = jnp.where(core0, mine[...], other[...])
    high = jnp.where(core0, other[...], mine[...])
    rank = jnp.concatenate([low, high], axis=1).reshape(blocks * share, LANES)
    _, degree, stuck = unpack(got)
    lost = jnp.sum(jnp.where(stuck, rank, 0.0))
    scaled = rank * jnp.where(stuck, 0.0, 1.0 / degree)
    total = products(scaled, select, keep, dest_ids, tiles, sources, rows * share)
    total = damping * (total + lost / pages)
    own_low = jnp.where(core0, mine[b], other[b])
    own_high = jnp.where(core0, other[b], mine[b])
    own = jnp.concatenate([own_low, own_high], axis=0)
    change = jnp.sum(jnp.abs(own - start[...]))
    own -= 1.0 - damping
    kept = jnp.zeros((share, LANES), jnp.float32)
    for r in range(rows):
        piece = total[r * share : (r + 1) * share]
        kept = jnp.where(w == r, piece, kept)
        less = jnp.where(w == r, piece - own, piece)
        for to in range(rows):
            send[to, r * share : (r + 1) * share] = less
    own_part[...] = kept
    for to in range(rows):
        send[to, rows * share :] = jnp.full((SCALAR_ROWS, LANES), change, jnp.float32)


def block_change(got, send):
    rows, height, _ = got.shape
    dest_tiles = height - SCALAR_ROWS
    total = got[0]
    for r in range(1, rows):
        total += got[r]
    change1 = jnp.sum(jnp.abs(total[:dest_tiles]))
    lane = lax.broadcasted_iota(jnp.int32, (1, LANES), 1)
    line = jnp.where(lane == 0, total[dest_tiles : dest_tiles + 1], change1)
    send[...] = jnp.broadcast_to(line, send.shape)


def finish(rows, got, own_part, changes, rank, out):
    share = rank.shape[0]
    w = lax.axis_index("row")
    total = own_part[...] + (1.0 - damping)
    for r in range(rows):
        total += jnp.where(w == r, 0.0, got[r, pl.ds(w * share, share), :])
    rank[...] = total
    out[...] = jnp.sum(changes[...], axis=0)[: out.shape[0]]


def local(rank_start, tiles, tile_dest, tile_src, tile_fill, out_degree, dangling):
    share, slots = rank_start.shape[0], tiles.shape[0]
    blocks, rows = lax.axis_size("blk"), lax.axis_size("row")
    half, dest_tiles = share // 2, rows * share
    pages = float(blocks * rows * share * LANES)
    f32 = functools.partial(jax.ShapeDtypeStruct, dtype=jnp.float32)
    sources = (pltpu.VMEM((slots, LANES), jnp.float32),)

    arguments = (rank_start, out_degree, dangling, tile_dest[None], tile_src[None], tile_fill[None])
    payload, *table, start = call(
        prepare,
        (
            jax.ShapeDtypeStruct((blocks, 2 * share, LANES), jnp.bfloat16),
            jax.ShapeDtypeStruct((slots, blocks * share), jnp.bfloat16),
            f32((slots, LANES)),
            jax.ShapeDtypeStruct((slots, LANES), jnp.int32),
            f32((share, LANES)),
        ),
        (*(pltpu.VMEM(a.shape, a.dtype) for a in arguments), pltpu.SemaphoreType.DMA((len(arguments),))),
        HBM,
        flops=1000000000,
    )(*(pltpu.with_memory_space_constraint(a, pltpu.HBM) for a in arguments))

    table = (*table, tiles)
    got_a = lax.all_to_all(payload, "blk", 0, 0)
    send = call(functools.partial(first, pages, rows), f32((blocks * rows, half, LANES)), sources)(got_a, *table)

    got_b = lax.all_to_all(send, ("blk", "row"), 0, 0)
    mine = call(functools.partial(gather_rows, rows), f32((blocks, half, LANES)))(got_b)
    other = lax.ppermute(mine, "blk", [(i, i ^ 1) for i in range(blocks)])
    send, own_part = call(
        functools.partial(second, pages, rows),
        (f32((rows, dest_tiles + SCALAR_ROWS, LANES)), f32((share, LANES))),
        sources,
    )(mine, other, got_a, start, *table)

    got_d = lax.all_to_all(send, "row", 0, 0)
    send = call(block_change, f32((blocks, LANES)))(got_d)

    got_e = lax.all_to_all(send, "blk", 0, 0, tiled=True)
    return call(functools.partial(finish, rows), (f32((share, LANES)), f32((2,))))(got_d, own_part, got_e)


def solution(mesh):
    placed = (
        P(("blk", "row"), None),
        P(("blk", "row"), None, None),
        P(("blk", "row")),
        P(("blk", "row")),
        P(("blk", "row")),
        P(("blk", "row"), None),
        P(("blk", "row"), None),
    )
    return jax.shard_map(
        local, mesh=mesh, in_specs=placed, out_specs=(P(("blk", "row"), None), P()), check_vma=False
    )
```

```python
import functools

import jax
import jax.numpy as jnp
from jax import lax
from jax.experimental import pallas as pl
from jax.experimental.pallas import tpu as pltpu
from jax.sharding import PartitionSpec as P

LANES = 128
SCALAR_ROWS = 8
FLAG = 32.0
damping = 0.85
VMEM = pl.BlockSpec(memory_space=pltpu.VMEM)
HBM = pl.BlockSpec(memory_space=pltpu.HBM)


def call(kernel, outs, scratch=(), space=VMEM, flops=1000000):
    def run(*arguments):
        return pl.pallas_call(
            kernel,
            out_shape=outs,
            in_specs=(space,) * len(arguments),
            out_specs=(VMEM,) * len(outs) if isinstance(outs, tuple) else VMEM,
            scratch_shapes=scratch,
            compiler_params=pltpu.CompilerParams(vmem_limit_bytes=24 * 1024 * 1024),
            cost_estimate=pl.CostEstimate(flops=flops, bytes_accessed=1000000, transcendentals=0),
        )(*arguments)

    return run


def column(row):
    n = row.shape[1]
    square = jnp.broadcast_to(row.astype(jnp.float32), (n, n))
    diagonal = lax.broadcasted_iota(jnp.int32, (n, n), 0) == lax.broadcasted_iota(jnp.int32, (n, n), 1)
    return jnp.sum(jnp.where(diagonal, square, 0.0), axis=1, keepdims=True)


def prepare(*refs):
    arguments, (payload, select, keep, dest_ids, start), scratch, sems = refs[:6], refs[6:11], refs[11:17], refs[17]
    copies = [
        pltpu.make_async_copy(source, target, sems.at[i])
        for i, (source, target) in enumerate(zip(arguments, scratch, strict=True))
    ]
    for copy in copies:
        copy.start()
    for copy in copies:
        copy.wait()
    rank, degree, dangling, dest, src, fill = scratch
    share = rank.shape[0]
    stuck = dangling[...] > 0
    degree, rank = degree[...].astype(jnp.float32), rank[...]
    scaled = (rank * (1.0 / degree)).astype(jnp.bfloat16).astype(jnp.float32)
    high = rank.astype(jnp.bfloat16).astype(jnp.float32)
    planes = [jnp.where(stuck, high, scaled), jnp.where(stuck, rank - high, degree)]
    for i, plane in enumerate(planes):
        rows = slice(i * share, (i + 1) * share)
        payload[:, rows] = jnp.broadcast_to(plane.astype(jnp.bfloat16)[None], (payload.shape[0], share, LANES))
    start[...] = rank
    lane = lax.broadcasted_iota(jnp.int32, select.shape, 1).astype(jnp.float32)
    select[...] = jnp.where(column(src[...]) == lane, 1.0, 0.0).astype(jnp.bfloat16)
    lane = lax.broadcasted_iota(jnp.int32, keep.shape, 1).astype(jnp.float32)
    keep[...] = jnp.where(lane < column(fill[...]), 1.0, 0.0)
    dest_ids[...] = jnp.broadcast_to(column(dest[...]), dest_ids.shape).astype(jnp.int32)


def unpack(got, order):
    share = got.shape[1] // 2
    place = [order.index(b) for b in range(len(order))]
    one = jnp.concatenate([got[p, :share] for p in place], axis=0).astype(jnp.float32)
    two = jnp.concatenate([got[p, share:] for p in place], axis=0).astype(jnp.float32)
    return one, two, two < FLAG


def products(scaled, select, keep, dest_ids, tiles, sources, dest_tiles):
    picked = jnp.dot(select[...], scaled.astype(jnp.bfloat16), preferred_element_type=jnp.float32)
    sources[...] = jnp.where(keep[...] > 0.0, picked, 0.0)
    target = lax.broadcasted_iota(jnp.int32, (dest_tiles, LANES), 0)
    total = jnp.zeros((dest_tiles, LANES), jnp.float32)
    slots = tiles.shape[0]
    together = 2 - slots % 2

    def placed(k):
        line = jnp.where(dest_ids[pl.ds(k, 1), :] == target, sources[pl.ds(k, 1), :], 0.0)
        return line.astype(jnp.bfloat16)

    for first_slot in range(0, slots, together):
        group = range(first_slot, first_slot + together)
        total += lax.dot_general(
            jnp.concatenate([placed(k) for k in group], axis=1),
            jnp.concatenate([tiles[k] for k in group], axis=1),
            (((1,), (1,)), ((), ())),
            preferred_element_type=jnp.float32,
        )
    return total


def first(pages, rows, order, members, got, select, keep, dest_ids, tiles, send, sources):
    share = got.shape[1] // 2
    one, two, stuck = unpack(got, order)
    lost = jnp.sum(jnp.where(stuck, one + two, 0.0))
    scaled = jnp.where(stuck, 0.0, one)
    total = products(scaled, select, keep, dest_ids, tiles, sources, rows * share) + lost / pages
    for i, (_, w) in enumerate(members):
        send[i] = total[w * share : (w + 1) * share]


def gather_rows(rows, members, got, mine):
    for pair in range(mine.shape[0]):
        total = got[members.index((pair, 0))]
        for w in range(1, rows):
            total += got[members.index((pair, w))]
        mine[pair] = damping * total + (1.0 - damping)


def second(pages, rows, order, mine, other, got, start, select, keep, dest_ids, tiles, send, own_part, sources):
    share = got.shape[1] // 2
    b, w = lax.axis_index("blk"), lax.axis_index("row")
    core0 = lax.rem(b, 2) == 0
    pieces = []
    for pair in range(mine.shape[0]):
        pieces.append(jnp.where(core0, mine[pair], other[pair]))
        pieces.append(jnp.where(core0, other[pair], mine[pair]))
    rank = jnp.concatenate(pieces, axis=0)
    _, degree, stuck = unpack(got, order)
    lost = jnp.sum(jnp.where(stuck, rank, 0.0))
    scaled = rank * jnp.where(stuck, 0.0, 1.0 / degree)
    total = products(scaled, select, keep, dest_ids, tiles, sources, rows * share)
    total = damping * (total + lost / pages)
    own = mine[lax.div(b, 2)]
    change = jnp.sum(jnp.abs(own - start[...]))
    own -= 1.0 - damping
    kept = jnp.zeros((share, LANES), jnp.float32)
    for r in range(rows):
        piece = total[r * share : (r + 1) * share]
        kept = jnp.where(w == r, piece, kept)
        less = jnp.where(w == r, piece - own, piece)
        for to in range(rows):
            send[to, r * share : (r + 1) * share] = less
    own_part[...] = kept
    for to in range(rows):
        send[to, rows * share :] = jnp.full((SCALAR_ROWS, LANES), change, jnp.float32)


def block_change(got, send):
    rows, height, _ = got.shape
    dest_tiles = height - SCALAR_ROWS
    total = got[0]
    for r in range(1, rows):
        total += got[r]
    change1 = jnp.sum(jnp.abs(total[:dest_tiles]))
    lane = lax.broadcasted_iota(jnp.int32, (1, LANES), 1)
    line = jnp.where(lane == 0, total[dest_tiles : dest_tiles + 1], change1)
    send[...] = jnp.broadcast_to(line, send.shape)


def finish(order, got, own_part, changes, rank, out):
    share = rank.shape[0]
    w = lax.axis_index("row")
    total = own_part[...] + (1.0 - damping)
    for i, r in enumerate(order):
        total += jnp.where(w == r, 0.0, got[i, pl.ds(w * share, share), :])
    rank[...] = total
    out[...] = jnp.sum(changes[...], axis=0)[: out.shape[0]]


def local(rank_start, tiles, tile_dest, tile_src, tile_fill, out_degree, dangling):
    share, slots = rank_start.shape[0], tiles.shape[0]
    blocks, rows = lax.axis_size("blk"), lax.axis_size("row")
    dest_tiles = rows * share
    by_block = list(range(blocks))[::-1]
    by_row = [rows // 2] + [w for w in range(rows) if w != rows // 2]
    members = [(pair, w) for w in by_row for pair in range(blocks // 2)[::-1]]
    pages = float(blocks * rows * share * LANES)
    f32 = functools.partial(jax.ShapeDtypeStruct, dtype=jnp.float32)
    sources = (pltpu.VMEM((slots, LANES), jnp.float32),)

    arguments = (rank_start, out_degree, dangling, tile_dest[None], tile_src[None], tile_fill[None])
    payload, *table, start = call(
        prepare,
        (
            jax.ShapeDtypeStruct((blocks, 2 * share, LANES), jnp.bfloat16),
            jax.ShapeDtypeStruct((slots, blocks * share), jnp.bfloat16),
            f32((slots, LANES)),
            jax.ShapeDtypeStruct((slots, LANES), jnp.int32),
            f32((share, LANES)),
        ),
        (*(pltpu.VMEM(a.shape, a.dtype) for a in arguments), pltpu.SemaphoreType.DMA((len(arguments),))),
        HBM,
        flops=1000000000,
    )(*(pltpu.with_memory_space_constraint(a, pltpu.HBM) for a in arguments))

    got_a = lax.all_to_all(payload, "blk", 0, 0, axis_index_groups=[by_block])
    table = (*table, tiles)
    send = call(functools.partial(first, pages, rows, by_block, members), f32((len(members), share, LANES)), sources)(
        got_a, *table
    )

    groups = [[(2 * pair + core) * rows + w for pair, w in members] for core in range(2)]
    got_b = lax.all_to_all(send, ("blk", "row"), 0, 0, axis_index_groups=groups)
    mine = call(functools.partial(gather_rows, rows, members), f32((blocks // 2, share, LANES)))(got_b)
    other = lax.ppermute(mine, "blk", [(i, i ^ 1) for i in range(blocks)])
    send, own_part = call(
        functools.partial(second, pages, rows, by_block),
        (f32((rows, dest_tiles + SCALAR_ROWS, LANES)), f32((share, LANES))),
        sources,
    )(mine, other, got_a, start, *table)

    got_d = lax.all_to_all(send, "row", 0, 0, axis_index_groups=[by_row])
    send = call(block_change, f32((blocks, LANES)))(got_d)

    got_e = lax.all_to_all(send, "blk", 0, 0, tiled=True, axis_index_groups=[by_block])
    return call(functools.partial(finish, by_row), (f32((share, LANES)), f32((2,))))(got_d, own_part, got_e)


def solution(mesh):
    placed = (
        P(("blk", "row"), None),
        P(("blk", "row"), None, None),
        P(("blk", "row")),
        P(("blk", "row")),
        P(("blk", "row")),
        P(("blk", "row"), None),
        P(("blk", "row"), None),
    )
    return jax.shard_map(
        local, mesh=mesh, in_specs=placed, out_specs=(P(("blk", "row"), None), P()), check_vma=False
    )
```

```python
import functools

import jax
import jax.numpy as jnp
from jax import lax
from jax.experimental import pallas as pl
from jax.experimental.pallas import tpu as pltpu
from jax.sharding import PartitionSpec as P

LANES = 128
SCALAR_ROWS = 8
FLAG = 32.0
damping = 0.85
VMEM = pl.BlockSpec(memory_space=pltpu.VMEM)
HBM = pl.BlockSpec(memory_space=pltpu.HBM)


def call(kernel, outs, scratch=(), space=VMEM, flops=1000000):
    def run(*arguments):
        return pl.pallas_call(
            kernel,
            out_shape=outs,
            in_specs=(space,) * len(arguments),
            out_specs=(VMEM,) * len(outs) if isinstance(outs, tuple) else VMEM,
            scratch_shapes=scratch,
            compiler_params=pltpu.CompilerParams(vmem_limit_bytes=24 * 1024 * 1024),
            cost_estimate=pl.CostEstimate(flops=flops, bytes_accessed=1000000, transcendentals=0),
        )(*arguments)

    return run


def column(row):
    n = row.shape[1]
    square = jnp.broadcast_to(row.astype(jnp.float32), (n, n))
    diagonal = lax.broadcasted_iota(jnp.int32, (n, n), 0) == lax.broadcasted_iota(jnp.int32, (n, n), 1)
    return jnp.sum(jnp.where(diagonal, square, 0.0), axis=1, keepdims=True)


def prepare(*refs):
    arguments, (payload, select, keep, dest_ids, start), scratch, sems = refs[:6], refs[6:11], refs[11:17], refs[17]
    copies = [
        pltpu.make_async_copy(source, target, sems.at[i])
        for i, (source, target) in enumerate(zip(arguments, scratch, strict=True))
    ]
    for copy in copies:
        copy.start()
    for copy in copies:
        copy.wait()
    rank, degree, dangling, dest, src, fill = scratch
    share = rank.shape[0]
    stuck = dangling[...] > 0
    degree, rank = degree[...].astype(jnp.float32), rank[...]
    scaled = (rank * (1.0 / degree)).astype(jnp.bfloat16).astype(jnp.float32)
    high = rank.astype(jnp.bfloat16).astype(jnp.float32)
    planes = [jnp.where(stuck, high, scaled), jnp.where(stuck, rank - high, degree)]
    for i, plane in enumerate(planes):
        rows = slice(i * share, (i + 1) * share)
        payload[:, rows] = jnp.broadcast_to(plane.astype(jnp.bfloat16)[None], (payload.shape[0], share, LANES))
    start[...] = rank
    lane = lax.broadcasted_iota(jnp.int32, select.shape, 1).astype(jnp.float32)
    select[...] = jnp.where(column(src[...]) == lane, 1.0, 0.0).astype(jnp.bfloat16)
    lane = lax.broadcasted_iota(jnp.int32, keep.shape, 1).astype(jnp.float32)
    keep[...] = jnp.where(lane < column(fill[...]), 1.0, 0.0)
    dest_ids[...] = jnp.broadcast_to(column(dest[...]), dest_ids.shape).astype(jnp.int32)


def unpack(got, order):
    share = got.shape[1] // 2
    place = [order.index(b) for b in range(len(order))]
    one = jnp.concatenate([got[p, :share] for p in place], axis=0).astype(jnp.float32)
    two = jnp.concatenate([got[p, share:] for p in place], axis=0).astype(jnp.float32)
    return one, two, two < FLAG


def products(scaled, select, keep, dest_ids, tiles, sources, dest_tiles, turned=False):
    picked = jnp.dot(select[...], scaled.astype(jnp.bfloat16), preferred_element_type=jnp.float32)
    sources[...] = jnp.where(keep[...] > 0.0, picked, 0.0)
    target = lax.broadcasted_iota(jnp.int32, (dest_tiles, LANES), 0)
    total = jnp.zeros((dest_tiles, LANES), jnp.float32)
    slots = tiles.shape[0]
    together = 2 - slots % 2

    def placed(k):
        line = jnp.where(dest_ids[pl.ds(k, 1), :] == target, sources[pl.ds(k, 1), :], 0.0)
        return line.astype(jnp.bfloat16)

    for first_slot in range(0, slots, together):
        group = range(first_slot, first_slot + together)
        total += lax.dot_general(
            jnp.concatenate([placed(k) for k in group], axis=1),
            jnp.concatenate([tiles[k] for k in group], axis=0 if turned else 1),
            (((1,), (0 if turned else 1,)), ((), ())),
            preferred_element_type=jnp.float32,
        )
    return total


def first(pages, rows, order, members, got, select, keep, dest_ids, tiles, send, sources):
    share = got.shape[1] // 2
    one, two, stuck = unpack(got, order)
    lost = jnp.sum(jnp.where(stuck, one + two, 0.0))
    scaled = jnp.where(stuck, 0.0, one)
    total = products(scaled, select, keep, dest_ids, tiles, sources, rows * share) + lost / pages
    for i, w in enumerate(members):
        send[i] = total[w * share : (w + 1) * share]


def gather_rows(rows, got, mine):
    slots = mine.shape[0]
    for i in range(slots):
        total = got[i]
        for r in range(1, rows):
            total += got[r * slots + i]
        mine[i] = damping * total + (1.0 - damping)


def block_class(b, pairs):
    return jnp.where(lax.div(b, 2) >= pairs // 2, 1 - lax.rem(b, 2), lax.rem(b, 2))


def slot_of(pair, kind, pairs):
    return (pair + (1 - kind) * (pairs // 2)) % pairs


def meanwhile(order, got, tiles, weight, flag, turned):
    _, degree, stuck = unpack(got, order)
    weight[...] = jnp.where(stuck, 0.0, 1.0 / degree)
    flag[...] = jnp.where(stuck, 1.0, 0.0)
    for k in range(tiles.shape[0]):
        turned[k] = tiles[k].T


def second(pages, rows, mine, other, weight, flag, start, select, keep, dest_ids, tiles, send, own_part, sources):
    share = mine.shape[1]
    b, w = lax.axis_index("blk"), lax.axis_index("row")
    pairs = mine.shape[0]
    kind = block_class(b, pairs)
    pieces = []
    for block in range(2 * pairs):
        its = 1 - block % 2 if block // 2 >= pairs // 2 else block % 2
        slot = slot_of(block // 2, its, pairs)
        pieces.append(jnp.where(kind == its, mine[slot], other[slot]))
    rank = jnp.concatenate(pieces, axis=0)
    lost = jnp.sum(rank * flag[...])
    scaled = rank * weight[...]
    total = products(scaled, select, keep, dest_ids, tiles, sources, rows * share, turned=True)
    total = damping * (total + lost / pages)
    own = mine[lax.rem(lax.div(b, 2) + (1 - kind) * (pairs // 2), pairs)]
    change = jnp.sum(jnp.abs(own - start[...]))
    own -= 1.0 - damping
    kept = jnp.zeros((share, LANES), jnp.float32)
    for r in range(rows):
        piece = total[r * share : (r + 1) * share]
        kept = jnp.where(w == r, piece, kept)
        less = jnp.where(w == r, piece - own, piece)
        for to in range(rows):
            send[to, r * share : (r + 1) * share] = less
    own_part[...] = kept
    for to in range(rows):
        send[to, rows * share :] = jnp.full((SCALAR_ROWS, LANES), change, jnp.float32)


def block_change(got, send):
    rows, height, _ = got.shape
    dest_tiles = height - SCALAR_ROWS
    total = got[0]
    for r in range(1, rows):
        total += got[r]
    change1 = jnp.sum(jnp.abs(total[:dest_tiles]))
    lane = lax.broadcasted_iota(jnp.int32, (1, LANES), 1)
    line = jnp.where(lane == 0, total[dest_tiles : dest_tiles + 1], change1)
    send[...] = jnp.broadcast_to(line, send.shape)


def finish(order, got, own_part, changes, rank, out):
    share = rank.shape[0]
    w = lax.axis_index("row")
    total = own_part[...] + (1.0 - damping)
    for i, r in enumerate(order):
        total += jnp.where(w == r, 0.0, got[i, pl.ds(w * share, share), :])
    rank[...] = total
    out[...] = jnp.sum(changes[...], axis=0)[: out.shape[0]]


def local(rank_start, tiles, tile_dest, tile_src, tile_fill, out_degree, dangling):
    share, slots = rank_start.shape[0], tiles.shape[0]
    blocks, rows = lax.axis_size("blk"), lax.axis_size("row")
    dest_tiles = rows * share
    by_block = list(range(blocks))[::-1]
    by_row = [rows // 2] + [w for w in range(rows) if w != rows // 2]
    members = [w for w in by_row for _ in range(blocks // 2)]
    pages = float(blocks * rows * share * LANES)
    f32 = functools.partial(jax.ShapeDtypeStruct, dtype=jnp.float32)
    sources = (pltpu.VMEM((slots, LANES), jnp.float32),)

    arguments = (rank_start, out_degree, dangling, tile_dest[None], tile_src[None], tile_fill[None])
    payload, *table, start = call(
        prepare,
        (
            jax.ShapeDtypeStruct((blocks, 2 * share, LANES), jnp.bfloat16),
            jax.ShapeDtypeStruct((slots, blocks * share), jnp.bfloat16),
            f32((slots, LANES)),
            jax.ShapeDtypeStruct((slots, LANES), jnp.int32),
            f32((share, LANES)),
        ),
        (*(pltpu.VMEM(a.shape, a.dtype) for a in arguments), pltpu.SemaphoreType.DMA((len(arguments),))),
        HBM,
        flops=1000000000,
    )(*(pltpu.with_memory_space_constraint(a, pltpu.HBM) for a in arguments))

    got_a = lax.all_to_all(payload, "blk", 0, 0, axis_index_groups=[by_block])
    table = (*table, tiles)
    send = call(functools.partial(first, pages, rows, by_block, members), f32((len(members), share, LANES)), sources)(
        got_a, *table
    )

    pairs = blocks // 2
    groups = [[None] * (pairs * rows) for _ in range(2)]
    for b in range(blocks):
        kind = 1 - b % 2 if b // 2 >= pairs // 2 else b % 2
        for i, w in enumerate(by_row):
            groups[kind][i * pairs + slot_of(b // 2, kind, pairs)] = b * rows + w
    got_b = lax.all_to_all(send, ("blk", "row"), 0, 0, axis_index_groups=groups)
    mine = call(functools.partial(gather_rows, rows), f32((pairs, share, LANES)))(got_b)
    other = lax.ppermute(mine, "blk", [(i, i ^ 1) for i in range(blocks)])
    weight, flag, turned = call(
        functools.partial(meanwhile, by_block),
        (f32((blocks * share, LANES)), f32((blocks * share, LANES)), jax.ShapeDtypeStruct(tiles.shape, tiles.dtype)),
    )(got_a, tiles)
    send, own_part = call(
        functools.partial(second, pages, rows),
        (f32((rows, dest_tiles + SCALAR_ROWS, LANES)), f32((share, LANES))),
        sources,
    )(mine, other, weight, flag, start, *table[:3], turned)

    got_d = lax.all_to_all(send, "row", 0, 0, axis_index_groups=[by_row])
    send = call(block_change, f32((blocks, LANES)))(got_d)

    got_e = lax.all_to_all(send, "blk", 0, 0, tiled=True, axis_index_groups=[by_block])
    return call(functools.partial(finish, by_row), (f32((share, LANES)), f32((2,))))(got_d, own_part, got_e)


def solution(mesh):
    placed = (
        P(("blk", "row"), None),
        P(("blk", "row"), None, None),
        P(("blk", "row")),
        P(("blk", "row")),
        P(("blk", "row")),
        P(("blk", "row"), None),
        P(("blk", "row"), None),
    )
    return jax.shard_map(
        local, mesh=mesh, in_specs=placed, out_specs=(P(("blk", "row"), None), P()), check_vma=False
    )
```

```python
import functools

import jax
import jax.numpy as jnp
from jax import lax
from jax.experimental import pallas as pl
from jax.experimental.pallas import tpu as pltpu
from jax.sharding import PartitionSpec as P

LANES = 128
SCALAR_ROWS = 8
FLAG = 32.0
damping = 0.85
VMEM = pl.BlockSpec(memory_space=pltpu.VMEM)
HBM = pl.BlockSpec(memory_space=pltpu.HBM)


def call(kernel, outs, scratch=(), space=VMEM, flops=1000000):
    def run(*arguments):
        return pl.pallas_call(
            kernel,
            out_shape=outs,
            in_specs=(space,) * len(arguments),
            out_specs=(VMEM,) * len(outs) if isinstance(outs, tuple) else VMEM,
            scratch_shapes=scratch,
            compiler_params=pltpu.CompilerParams(vmem_limit_bytes=24 * 1024 * 1024),
            cost_estimate=pl.CostEstimate(flops=flops, bytes_accessed=1000000, transcendentals=0),
        )(*arguments)

    return run


def column(row):
    n = row.shape[1]
    square = jnp.broadcast_to(row.astype(jnp.float32), (n, n))
    diagonal = lax.broadcasted_iota(jnp.int32, (n, n), 0) == lax.broadcasted_iota(jnp.int32, (n, n), 1)
    return jnp.sum(jnp.where(diagonal, square, 0.0), axis=1, keepdims=True)


def prepare(*refs):
    arguments, (payload, select, keep, dest_ids, start), scratch, sems = refs[:6], refs[6:11], refs[11:17], refs[17]
    copies = [
        pltpu.make_async_copy(source, target, sems.at[i])
        for i, (source, target) in enumerate(zip(arguments, scratch, strict=True))
    ]
    for copy in copies:
        copy.start()
    for copy in copies:
        copy.wait()
    rank, degree, dangling, dest, src, fill = scratch
    share = rank.shape[0]
    stuck = dangling[...] > 0
    degree, rank = degree[...].astype(jnp.float32), rank[...]
    scaled = (rank * (1.0 / degree)).astype(jnp.bfloat16).astype(jnp.float32)
    high = rank.astype(jnp.bfloat16).astype(jnp.float32)
    planes = [jnp.where(stuck, high, scaled), jnp.where(stuck, rank - high, degree)]
    for i, plane in enumerate(planes):
        rows = slice(i * share, (i + 1) * share)
        payload[:, rows] = jnp.broadcast_to(plane.astype(jnp.bfloat16)[None], (payload.shape[0], share, LANES))
    start[...] = rank
    lane = lax.broadcasted_iota(jnp.int32, select.shape, 1).astype(jnp.float32)
    select[...] = jnp.where(column(src[...]) == lane, 1.0, 0.0).astype(jnp.bfloat16)
    lane = lax.broadcasted_iota(jnp.int32, keep.shape, 1).astype(jnp.float32)
    keep[...] = jnp.where(lane < column(fill[...]), 1.0, 0.0)
    dest_ids[...] = jnp.broadcast_to(column(dest[...]), dest_ids.shape).astype(jnp.int32)


def unpack(got, order):
    share = got.shape[1] // 2
    place = [order.index(b) for b in range(len(order))]
    one = jnp.concatenate([got[p, :share] for p in place], axis=0).astype(jnp.float32)
    two = jnp.concatenate([got[p, share:] for p in place], axis=0).astype(jnp.float32)
    return one, two, two < FLAG


def products(scaled, select, keep, dest_ids, tiles, sources, dest_tiles, turned=False):
    picked = jnp.dot(select[...], scaled.astype(jnp.bfloat16), preferred_element_type=jnp.float32)
    sources[...] = jnp.where(keep[...] > 0.0, picked, 0.0)
    target = lax.broadcasted_iota(jnp.int32, (dest_tiles, LANES), 0)
    total = jnp.zeros((dest_tiles, LANES), jnp.float32)
    slots = tiles.shape[0]
    together = 2 - slots % 2

    def placed(k):
        line = jnp.where(dest_ids[pl.ds(k, 1), :] == target, sources[pl.ds(k, 1), :], 0.0)
        return line.astype(jnp.bfloat16)

    for first_slot in range(0, slots, together):
        group = range(first_slot, first_slot + together)
        total += lax.dot_general(
            jnp.concatenate([placed(k) for k in group], axis=1),
            jnp.concatenate([tiles[k] for k in group], axis=0 if turned else 1),
            (((1,), (0 if turned else 1,)), ((), ())),
            preferred_element_type=jnp.float32,
        )
    return total


def first(pages, rows, order, members, got, select, keep, dest_ids, tiles, send, sources):
    share = got.shape[1] // 2
    one, two, stuck = unpack(got, order)
    lost = jnp.sum(jnp.where(stuck, one + two, 0.0))
    scaled = jnp.where(stuck, 0.0, one)
    total = products(scaled, select, keep, dest_ids, tiles, sources, rows * share) + lost / pages
    for i, (_, w) in enumerate(members):
        send[i] = total[w * share : (w + 1) * share]


def gather_rows(rows, members, got, mine):
    for pair in range(mine.shape[0]):
        total = got[members.index((pair, 0))]
        for w in range(1, rows):
            total += got[members.index((pair, w))]
        mine[pair] = damping * total + (1.0 - damping)


def meanwhile(order, got, tiles, weight, flag, turned):
    _, degree, stuck = unpack(got, order)
    weight[...] = jnp.where(stuck, 0.0, 1.0 / degree)
    flag[...] = jnp.where(stuck, 1.0, 0.0)
    for k in range(tiles.shape[0]):
        turned[k] = tiles[k].T


def second(pages, rows, mine, other, weight, flag, start, select, keep, dest_ids, tiles, send, own_part, sources):
    share = mine.shape[1]
    b, w = lax.axis_index("blk"), lax.axis_index("row")
    core0 = lax.rem(b, 2) == 0
    pieces = []
    for pair in range(mine.shape[0]):
        pieces.append(jnp.where(core0, mine[pair], other[pair]))
        pieces.append(jnp.where(core0, other[pair], mine[pair]))
    rank = jnp.concatenate(pieces, axis=0)
    lost = jnp.sum(rank * flag[...])
    scaled = rank * weight[...]
    total = products(scaled, select, keep, dest_ids, tiles, sources, rows * share, turned=True)
    total = damping * (total + lost / pages)
    own = mine[lax.div(b, 2)]
    change = jnp.sum(jnp.abs(own - start[...]))
    own -= 1.0 - damping
    kept = jnp.zeros((share, LANES), jnp.float32)
    for r in range(rows):
        piece = total[r * share : (r + 1) * share]
        kept = jnp.where(w == r, piece, kept)
        less = jnp.where(w == r, piece - own, piece)
        for to in range(rows):
            send[to, r * share : (r + 1) * share] = less
    own_part[...] = kept
    for to in range(rows):
        send[to, rows * share :] = jnp.full((SCALAR_ROWS, LANES), change, jnp.float32)


def block_change(got, send):
    rows, height, _ = got.shape
    dest_tiles = height - SCALAR_ROWS
    total = got[0]
    for r in range(1, rows):
        total += got[r]
    change1 = jnp.sum(jnp.abs(total[:dest_tiles]))
    lane = lax.broadcasted_iota(jnp.int32, (1, LANES), 1)
    line = jnp.where(lane == 0, total[dest_tiles : dest_tiles + 1], change1)
    send[...] = jnp.broadcast_to(line, send.shape)


def finish(order, got, own_part, changes, rank, out):
    share = rank.shape[0]
    w = lax.axis_index("row")
    total = own_part[...] + (1.0 - damping)
    for i, r in enumerate(order):
        total += jnp.where(w == r, 0.0, got[i, pl.ds(w * share, share), :])
    rank[...] = total
    out[...] = jnp.sum(changes[...], axis=0)[: out.shape[0]]


def local(rank_start, tiles, tile_dest, tile_src, tile_fill, out_degree, dangling):
    share, slots = rank_start.shape[0], tiles.shape[0]
    blocks, rows = lax.axis_size("blk"), lax.axis_size("row")
    dest_tiles = rows * share
    by_block = list(range(blocks))[::-1]
    by_row = [*range(rows // 2, rows), *range(rows // 2)[::-1]]
    members = [(pair, w) for w in by_row for pair in range(blocks // 2)[::-1]]
    pages = float(blocks * rows * share * LANES)
    f32 = functools.partial(jax.ShapeDtypeStruct, dtype=jnp.float32)
    sources = (pltpu.VMEM((slots, LANES), jnp.float32),)

    arguments = (rank_start, out_degree, dangling, tile_dest[None], tile_src[None], tile_fill[None])
    payload, *table, start = call(
        prepare,
        (
            jax.ShapeDtypeStruct((blocks, 2 * share, LANES), jnp.bfloat16),
            jax.ShapeDtypeStruct((slots, blocks * share), jnp.bfloat16),
            f32((slots, LANES)),
            jax.ShapeDtypeStruct((slots, LANES), jnp.int32),
            f32((share, LANES)),
        ),
        (*(pltpu.VMEM(a.shape, a.dtype) for a in arguments), pltpu.SemaphoreType.DMA((len(arguments),))),
        HBM,
        flops=1000000000,
    )(*(pltpu.with_memory_space_constraint(a, pltpu.HBM) for a in arguments))

    got_a = lax.all_to_all(payload, "blk", 0, 0, axis_index_groups=[by_block])
    table = (*table, tiles)
    send = call(functools.partial(first, pages, rows, by_block, members), f32((len(members), share, LANES)), sources)(
        got_a, *table
    )

    groups = [[(2 * pair + core) * rows + w for pair, w in members] for core in range(2)]
    got_b = lax.all_to_all(send, ("blk", "row"), 0, 0, axis_index_groups=groups)
    mine = call(functools.partial(gather_rows, rows, members), f32((blocks // 2, share, LANES)))(got_b)
    other = lax.ppermute(mine, "blk", [(i, i ^ 1) for i in range(blocks)])
    weight, flag, turned = call(
        functools.partial(meanwhile, by_block),
        (f32((blocks * share, LANES)), f32((blocks * share, LANES)), jax.ShapeDtypeStruct(tiles.shape, tiles.dtype)),
    )(got_a, tiles)
    send, own_part = call(
        functools.partial(second, pages, rows),
        (f32((rows, dest_tiles + SCALAR_ROWS, LANES)), f32((share, LANES))),
        sources,
    )(mine, other, weight, flag, start, *table[:3], turned)

    got_d = lax.all_to_all(send, "row", 0, 0, axis_index_groups=[by_row])
    send = call(block_change, f32((blocks, LANES)))(got_d)

    got_e = lax.all_to_all(send, "blk", 0, 0, tiled=True, axis_index_groups=[by_block])
    return call(functools.partial(finish, by_row), (f32((share, LANES)), f32((2,))))(got_d, own_part, got_e)


def solution(mesh):
    placed = (
        P(("blk", "row"), None),
        P(("blk", "row"), None, None),
        P(("blk", "row")),
        P(("blk", "row")),
        P(("blk", "row")),
        P(("blk", "row"), None),
        P(("blk", "row"), None),
    )
    return jax.shard_map(
        local, mesh=mesh, in_specs=placed, out_specs=(P(("blk", "row"), None), P()), check_vma=False
    )
```

```python
import functools

import jax
import jax.numpy as jnp
from jax import lax
from jax.experimental import pallas as pl
from jax.experimental.pallas import tpu as pltpu
from jax.sharding import PartitionSpec as P

LANES = 128
SCALAR_ROWS = 8
FLAG = 32.0
damping = 0.85
VMEM = pl.BlockSpec(memory_space=pltpu.VMEM)
HBM = pl.BlockSpec(memory_space=pltpu.HBM)
SMEM = pl.BlockSpec(memory_space=pltpu.SMEM)


def call(kernel, outs, scratch=(), space=VMEM, flops=1000000, scalars=(), scalar_outs=()):
    def run(*arguments):
        return pl.pallas_call(
            kernel,
            out_shape=outs,
            in_specs=[SMEM if i in scalars else space for i in range(len(arguments))],
            out_specs=tuple(SMEM if i in scalar_outs else VMEM for i in range(len(outs))) if isinstance(outs, tuple) else VMEM,
            scratch_shapes=scratch,
            compiler_params=pltpu.CompilerParams(vmem_limit_bytes=24 * 1024 * 1024),
            cost_estimate=pl.CostEstimate(flops=flops, bytes_accessed=1000000, transcendentals=0),
        )(*arguments)

    return run


def prepare(*refs):
    arguments, (payload, start, dest, src, fill), (degree, dangling, sems) = refs[:6], refs[6:11], refs[11:]
    copies = [
        pltpu.make_async_copy(source, target, sems.at[i])
        for i, (source, target) in enumerate(zip(arguments, (start, degree, dangling, dest, src, fill), strict=True))
    ]
    for copy in copies:
        copy.start()
    for copy in copies:
        copy.wait()
    share = start.shape[0]
    stuck = dangling[...] > 0
    degree, rank = degree[...].astype(jnp.float32), start[...]
    scaled = (rank * (1.0 / degree)).astype(jnp.bfloat16).astype(jnp.float32)
    high = rank.astype(jnp.bfloat16).astype(jnp.float32)
    planes = [jnp.where(stuck, high, scaled), jnp.where(stuck, rank - high, degree)]
    for i, plane in enumerate(planes):
        rows = slice(i * share, (i + 1) * share)
        payload[:, rows] = jnp.broadcast_to(plane.astype(jnp.bfloat16)[None], (payload.shape[0], share, LANES))


def unpack(got, order):
    share = got.shape[1] // 2
    place = [order.index(b) for b in range(len(order))]
    one = jnp.concatenate([got[p, :share] for p in place], axis=0).astype(jnp.float32)
    two = jnp.concatenate([got[p, share:] for p in place], axis=0).astype(jnp.float32)
    return one, two, two < FLAG


def products(scaled, dest, src, fill, tiles, pages_read, dest_tiles, turned=False):
    pages_read[...] = scaled.astype(jnp.bfloat16).astype(jnp.float32)
    target = lax.broadcasted_iota(jnp.int32, (dest_tiles, LANES), 0)
    lane = lax.broadcasted_iota(jnp.int32, (1, LANES), 1)
    total = jnp.zeros((dest_tiles, LANES), jnp.float32)
    slots = tiles.shape[0]
    together = 2 - slots % 2

    def placed(k):
        source = jnp.where(lane < fill[0, k], pages_read[pl.ds(src[0, k], 1), :], 0.0)
        return jnp.where(target == dest[0, k], source, 0.0).astype(jnp.bfloat16)

    for first_slot in range(0, slots, together):
        group = range(first_slot, first_slot + together)
        total += lax.dot_general(
            jnp.concatenate([placed(k) for k in group], axis=1),
            jnp.concatenate([tiles[k] for k in group], axis=0 if turned else 1),
            (((1,), (0 if turned else 1,)), ((), ())),
            preferred_element_type=jnp.float32,
        )
    return total


def first(pages, rows, order, members, got, dest, src, fill, tiles, send, pages_read):
    share = got.shape[1] // 2
    one, two, stuck = unpack(got, order)
    lost = jnp.sum(jnp.where(stuck, one + two, 0.0))
    scaled = jnp.where(stuck, 0.0, one)
    total = products(scaled, dest, src, fill, tiles, pages_read, rows * share) + lost / pages
    for i, (_, w) in enumerate(members):
        send[i] = total[w * share : (w + 1) * share]


def gather_rows(rows, members, got, mine):
    for pair in range(mine.shape[0]):
        total = got[members.index((pair, 0))]
        for w in range(1, rows):
            total += got[members.index((pair, w))]
        mine[pair] = damping * total + (1.0 - damping)


def meanwhile(order, got, tiles, weight, flag, turned):
    _, degree, stuck = unpack(got, order)
    weight[...] = jnp.where(stuck, 0.0, 1.0 / degree)
    flag[...] = jnp.where(stuck, 1.0, 0.0)
    for k in range(tiles.shape[0]):
        turned[k] = tiles[k].T


def second(pages, rows, mine, other, weight, flag, start, dest, src, fill, tiles, send, own_part, pages_read):
    share = mine.shape[1]
    b, w = lax.axis_index("blk"), lax.axis_index("row")
    core0 = lax.rem(b, 2) == 0
    pieces = []
    for pair in range(mine.shape[0]):
        pieces.append(jnp.where(core0, mine[pair], other[pair]))
        pieces.append(jnp.where(core0, other[pair], mine[pair]))
    rank = jnp.concatenate(pieces, axis=0)
    lost = jnp.sum(rank * flag[...])
    scaled = rank * weight[...]
    total = products(scaled, dest, src, fill, tiles, pages_read, rows * share, turned=True)
    total = damping * (total + lost / pages)
    own = mine[lax.div(b, 2)]
    change = jnp.sum(jnp.abs(own - start[...]))
    own -= 1.0 - damping
    kept = jnp.zeros((share, LANES), jnp.float32)
    for r in range(rows):
        piece = total[r * share : (r + 1) * share]
        kept = jnp.where(w == r, piece, kept)
        less = jnp.where(w == r, piece - own, piece)
        for to in range(rows):
            send[to, r * share : (r + 1) * share] = less
    own_part[...] = kept
    for to in range(rows):
        send[to, rows * share :] = jnp.full((SCALAR_ROWS, LANES), change, jnp.float32)


def block_change(got, send):
    rows, height, _ = got.shape
    dest_tiles = height - SCALAR_ROWS
    total = got[0]
    for r in range(1, rows):
        total += got[r]
    change1 = jnp.sum(jnp.abs(total[:dest_tiles]))
    lane = lax.broadcasted_iota(jnp.int32, (1, LANES), 1)
    line = jnp.where(lane == 0, total[dest_tiles : dest_tiles + 1], change1)
    send[...] = jnp.broadcast_to(line, send.shape)


def finish(order, got, own_part, changes, rank, out):
    share = rank.shape[0]
    w = lax.axis_index("row")
    total = own_part[...] + (1.0 - damping)
    for i, r in enumerate(order):
        total += jnp.where(w == r, 0.0, got[i, pl.ds(w * share, share), :])
    rank[...] = total
    out[...] = jnp.sum(changes[...], axis=0)[: out.shape[0]]


def local(rank_start, tiles, tile_dest, tile_src, tile_fill, out_degree, dangling):
    share, slots = rank_start.shape[0], tiles.shape[0]
    blocks, rows = lax.axis_size("blk"), lax.axis_size("row")
    dest_tiles = rows * share
    by_block = list(range(blocks))[::-1]
    by_row = [*range(rows // 2, rows), *range(rows // 2)[::-1]]
    members = [(pair, w) for w in by_row for pair in range(blocks // 2)[::-1]]
    pages = float(blocks * rows * share * LANES)
    f32 = functools.partial(jax.ShapeDtypeStruct, dtype=jnp.float32)
    pages_read = (pltpu.VMEM((blocks * share, LANES), jnp.float32),)

    arguments = (rank_start, out_degree, dangling, tile_dest[None], tile_src[None], tile_fill[None])
    whole, line = (share, LANES), pltpu.SMEM((1, slots), jnp.int32)
    payload, start, *table = call(
        prepare,
        (jax.ShapeDtypeStruct((blocks, 2 * share, LANES), jnp.bfloat16), f32(whole), line, line, line),
        (pltpu.VMEM(whole, jnp.int32), pltpu.VMEM(whole, jnp.int32), pltpu.SemaphoreType.DMA((len(arguments),))),
        HBM,
        flops=1000000000,
        scalar_outs=(2, 3, 4),
    )(*(pltpu.with_memory_space_constraint(a, pltpu.HBM) for a in arguments))
    table = [pltpu.with_memory_space_constraint(a, pltpu.SMEM) for a in table]

    got_a = lax.all_to_all(payload, "blk", 0, 0, axis_index_groups=[by_block])
    send = call(
        functools.partial(first, pages, rows, by_block, members),
        f32((len(members), share, LANES)),
        pages_read,
        scalars=(1, 2, 3),
    )(got_a, *table, tiles)

    groups = [[(2 * pair + core) * rows + w for pair, w in members] for core in range(2)]
    got_b = lax.all_to_all(send, ("blk", "row"), 0, 0, axis_index_groups=groups)
    mine = call(functools.partial(gather_rows, rows, members), f32((blocks // 2, share, LANES)))(got_b)
    other = lax.ppermute(mine, "blk", [(i, i ^ 1) for i in range(blocks)])
    weight, flag, turned = call(
        functools.partial(meanwhile, by_block),
        (f32((blocks * share, LANES)), f32((blocks * share, LANES)), jax.ShapeDtypeStruct(tiles.shape, tiles.dtype)),
    )(got_a, tiles)
    send, own_part = call(
        functools.partial(second, pages, rows),
        (f32((rows, dest_tiles + SCALAR_ROWS, LANES)), f32((share, LANES))),
        pages_read,
        scalars=(5, 6, 7),
    )(mine, other, weight, flag, start, *table, turned)

    got_d = lax.all_to_all(send, "row", 0, 0, axis_index_groups=[by_row])
    send = call(block_change, f32((blocks, LANES)))(got_d)

    got_e = lax.all_to_all(send, "blk", 0, 0, tiled=True, axis_index_groups=[by_block])
    return call(functools.partial(finish, by_row), (f32((share, LANES)), f32((2,))))(got_d, own_part, got_e)


def solution(mesh):
    placed = (
        P(("blk", "row"), None),
        P(("blk", "row"), None, None),
        P(("blk", "row")),
        P(("blk", "row")),
        P(("blk", "row")),
        P(("blk", "row"), None),
        P(("blk", "row"), None),
    )
    return jax.shard_map(
        local, mesh=mesh, in_specs=placed, out_specs=(P(("blk", "row"), None), P()), check_vma=False
    )
```

```python
import functools
import math

import jax
import jax.numpy as jnp
from jax import lax
from jax.experimental import pallas as pl
from jax.experimental.pallas import tpu as pltpu
from jax.sharding import PartitionSpec as P

LANES = 128
SCALAR_ROWS = 8
FLAG = 32.0
damping = 0.85
VMEM = pl.BlockSpec(memory_space=pltpu.VMEM)
HBM = pl.BlockSpec(memory_space=pltpu.HBM)
SMEM = pl.BlockSpec(memory_space=pltpu.SMEM)


def call(kernel, outs, scratch=(), space=VMEM, flops=1000000, scalars=(), scalar_outs=(), flags=None):
    def run(*arguments):
        return pl.pallas_call(
            kernel,
            out_shape=outs,
            in_specs=[SMEM if i in scalars else space for i in range(len(arguments))],
            out_specs=tuple(SMEM if i in scalar_outs else VMEM for i in range(len(outs))) if isinstance(outs, tuple) else VMEM,
            scratch_shapes=scratch,
            compiler_params=pltpu.CompilerParams(vmem_limit_bytes=24 * 1024 * 1024, flags=flags),
            cost_estimate=pl.CostEstimate(flops=flops, bytes_accessed=1000000, transcendentals=0),
        )(*arguments)

    return run


def prepare(*refs):
    arguments, (payload, start, dest, src, fill), (degree, dangling, sems) = refs[:6], refs[6:11], refs[11:]
    copies = [
        pltpu.make_async_copy(source, target, sems.at[i])
        for i, (source, target) in enumerate(zip(arguments, (start, degree, dangling, dest, src, fill), strict=True))
    ]
    for copy in copies:
        copy.start()
    for copy in copies:
        copy.wait()
    share = start.shape[0]
    stuck = dangling[...] > 0
    degree, rank = degree[...].astype(jnp.float32), start[...]
    scaled = (rank * (1.0 / degree)).astype(jnp.bfloat16).astype(jnp.float32)
    high = rank.astype(jnp.bfloat16).astype(jnp.float32)
    planes = [jnp.where(stuck, high, scaled), jnp.where(stuck, rank - high, degree)]
    for i, plane in enumerate(planes):
        rows = slice(i * share, (i + 1) * share)
        payload[:, rows] = jnp.broadcast_to(plane.astype(jnp.bfloat16)[None], (payload.shape[0], share, LANES))


def unpack(got, order):
    share = got.shape[1] // 2
    place = [order.index(b) for b in range(len(order))]
    one = jnp.concatenate([got[p, :share] for p in place], axis=0).astype(jnp.float32)
    two = jnp.concatenate([got[p, share:] for p in place], axis=0).astype(jnp.float32)
    return one, two, two < FLAG


def products_by_row(scaled, dest, src, fill, tiles, pages_read, sums):
    pages_read[...] = scaled.astype(jnp.bfloat16).astype(jnp.float32)
    sums[...] = jnp.zeros_like(sums)
    slots = tiles.shape[0]
    together = math.gcd(slots, 2)
    row = lax.broadcasted_iota(jnp.int32, (8, LANES), 0)
    lane = lax.broadcasted_iota(jnp.int32, (8, LANES), 1)
    for first_slot in range(0, slots, together):
        group = range(first_slot, first_slot + together)
        sources = [
            jnp.where((row == i) & (lane < fill[0, k]), pages_read[pl.ds(src[0, k], 1), :], 0.0)
            for i, k in enumerate(group)
        ]
        product = lax.dot_general(
            jnp.concatenate(sources, axis=1).astype(jnp.bfloat16),
            jnp.concatenate([tiles[k] for k in group], axis=1),
            (((1,), (1,)), ((), ())),
            preferred_element_type=jnp.float32,
        )
        for i, k in enumerate(group):
            sums[pl.ds(dest[0, k], 1), :] += product[i : i + 1]
    return sums[...]


def products_turned(scaled, dest, src, fill, turned, pages_read, dest_tiles):
    pages_read[...] = scaled.astype(jnp.bfloat16).astype(jnp.float32)
    target = lax.broadcasted_iota(jnp.int32, (dest_tiles, LANES), 0)
    lane = lax.broadcasted_iota(jnp.int32, (1, LANES), 1)
    total = jnp.zeros((dest_tiles, LANES), jnp.float32)
    slots = turned.shape[0]
    together = math.gcd(slots, 4)

    def placed(k):
        source = jnp.where(lane < fill[0, k], pages_read[pl.ds(src[0, k], 1), :], 0.0)
        return jnp.where(target == dest[0, k], source, 0.0).astype(jnp.bfloat16)

    for first_slot in range(0, slots, together):
        group = range(first_slot, first_slot + together)
        total += jnp.dot(
            jnp.concatenate([placed(k) for k in group], axis=1),
            jnp.concatenate([turned[k] for k in group], axis=0),
            preferred_element_type=jnp.float32,
        )
    return total


def first(pages, rows, order, members, got, dest, src, fill, tiles, send, pages_read, sums):
    share = got.shape[1] // 2
    one, two, stuck = unpack(got, order)
    lost = jnp.sum(jnp.where(stuck, one + two, 0.0))
    scaled = jnp.where(stuck, 0.0, one)
    total = products_by_row(scaled, dest, src, fill, tiles, pages_read, sums) + lost / pages
    for i, (_, w) in enumerate(members):
        send[i] = total[w * share : (w + 1) * share]


def gather_rows(rows, members, got, mine):
    for pair in range(mine.shape[0]):
        total = got[members.index((pair, 0))]
        for w in range(1, rows):
            total += got[members.index((pair, w))]
        mine[pair] = damping * total + (1.0 - damping)


def meanwhile(order, got, tiles, weight, flag, turned):
    _, degree, stuck = unpack(got, order)
    weight[...] = jnp.where(stuck, 0.0, 1.0 / degree)
    flag[...] = jnp.where(stuck, 1.0, 0.0)
    for k in range(tiles.shape[0]):
        turned[k] = tiles[k].T


def second(pages, rows, mine, other, weight, flag, start, dest, src, fill, turned, send, own_part, pages_read):
    share = mine.shape[1]
    b, w = lax.axis_index("blk"), lax.axis_index("row")
    core0 = lax.rem(b, 2) == 0
    pieces = []
    for pair in range(mine.shape[0]):
        pieces.append(jnp.where(core0, mine[pair], other[pair]))
        pieces.append(jnp.where(core0, other[pair], mine[pair]))
    rank = jnp.concatenate(pieces, axis=0)
    lost = jnp.sum(rank * flag[...])
    scaled = rank * weight[...]
    total = products_turned(scaled, dest, src, fill, turned, pages_read, rows * share)
    total = damping * (total + lost / pages)
    own = mine[lax.div(b, 2)]
    change = jnp.sum(jnp.abs(own - start[...]))
    own -= 1.0 - damping
    kept = jnp.zeros((share, LANES), jnp.float32)
    for r in range(rows):
        piece = total[r * share : (r + 1) * share]
        kept = jnp.where(w == r, piece, kept)
        less = jnp.where(w == r, piece - own, piece)
        for to in range(rows):
            send[to, r * share : (r + 1) * share] = less
    own_part[...] = kept
    for to in range(rows):
        send[to, rows * share :] = jnp.full((SCALAR_ROWS, LANES), change, jnp.float32)


def block_change(got, send):
    rows, height, _ = got.shape
    dest_tiles = height - SCALAR_ROWS
    total = got[0]
    for r in range(1, rows):
        total += got[r]
    change1 = jnp.sum(jnp.abs(total[:dest_tiles]))
    lane = lax.broadcasted_iota(jnp.int32, (1, LANES), 1)
    line = jnp.where(lane == 0, total[dest_tiles : dest_tiles + 1], change1)
    send[...] = jnp.broadcast_to(line, send.shape)


def finish(order, got, own_part, changes, rank, out):
    share = rank.shape[0]
    w = lax.axis_index("row")
    total = own_part[...] + (1.0 - damping)
    for i, r in enumerate(order):
        total += jnp.where(w == r, 0.0, got[i, pl.ds(w * share, share), :])
    rank[...] = total
    out[...] = jnp.sum(changes[...], axis=0)[: out.shape[0]]


def local(rank_start, tiles, tile_dest, tile_src, tile_fill, out_degree, dangling):
    share, slots = rank_start.shape[0], tiles.shape[0]
    blocks, rows = lax.axis_size("blk"), lax.axis_size("row")
    dest_tiles = rows * share
    by_block = list(range(blocks))[::-1]
    by_row = [*range(rows // 2, rows), *range(rows // 2)[::-1]]
    members = [(pair, w) for w in by_row for pair in range(blocks // 2)[::-1]]
    pages = float(blocks * rows * share * LANES)
    f32 = functools.partial(jax.ShapeDtypeStruct, dtype=jnp.float32)
    pages_read = (pltpu.VMEM((blocks * share, LANES), jnp.float32),)

    arguments = (rank_start, out_degree, dangling, tile_dest[None], tile_src[None], tile_fill[None])
    whole, line = (share, LANES), pltpu.SMEM((1, slots), jnp.int32)
    payload, start, *table = call(
        prepare,
        (jax.ShapeDtypeStruct((blocks, 2 * share, LANES), jnp.bfloat16), f32(whole), line, line, line),
        (pltpu.VMEM(whole, jnp.int32), pltpu.VMEM(whole, jnp.int32), pltpu.SemaphoreType.DMA((len(arguments),))),
        HBM,
        flops=1000000000,
        scalar_outs=(2, 3, 4),
    )(*(pltpu.with_memory_space_constraint(a, pltpu.HBM) for a in arguments))
    table = [pltpu.with_memory_space_constraint(a, pltpu.SMEM) for a in table]

    got_a = lax.all_to_all(payload, "blk", 0, 0, axis_index_groups=[by_block])
    send = call(
        functools.partial(first, pages, rows, by_block, members),
        f32((len(members), share, LANES)),
        (*pages_read, pltpu.VMEM((dest_tiles, LANES), jnp.float32)),
        scalars=(1, 2, 3),
    )(got_a, *table, tiles)

    groups = [[(2 * pair + core) * rows + w for pair, w in members] for core in range(2)]
    got_b = lax.all_to_all(send, ("blk", "row"), 0, 0, axis_index_groups=groups)
    mine = call(functools.partial(gather_rows, rows, members), f32((blocks // 2, share, LANES)))(got_b)
    other = lax.ppermute(mine, "blk", [(i, i ^ 1) for i in range(blocks)])
    weight, flag, turned = call(
        functools.partial(meanwhile, by_block),
        (f32((blocks * share, LANES)), f32((blocks * share, LANES)), jax.ShapeDtypeStruct(tiles.shape, tiles.dtype)),
    )(got_a, tiles)
    send, own_part = call(
        functools.partial(second, pages, rows),
        (f32((rows, dest_tiles + SCALAR_ROWS, LANES)), f32((share, LANES))),
        pages_read,
        scalars=(5, 6, 7),
    )(mine, other, weight, flag, start, *table, turned)

    got_d = lax.all_to_all(send, "row", 0, 0, axis_index_groups=[by_row])
    send = call(block_change, f32((blocks, LANES)))(got_d)

    got_e = lax.all_to_all(send, "blk", 0, 0, tiled=True, axis_index_groups=[by_block])
    return call(functools.partial(finish, by_row), (f32((share, LANES)), f32((2,))))(got_d, own_part, got_e)


def solution(mesh):
    placed = (
        P(("blk", "row"), None),
        P(("blk", "row"), None, None),
        P(("blk", "row")),
        P(("blk", "row")),
        P(("blk", "row")),
        P(("blk", "row"), None),
        P(("blk", "row"), None),
    )
    return jax.shard_map(
        local, mesh=mesh, in_specs=placed, out_specs=(P(("blk", "row"), None), P()), check_vma=False
    )
```

```python
import functools
import math

import jax
import jax.numpy as jnp
from jax import lax
from jax.experimental import pallas as pl
from jax.experimental.pallas import tpu as pltpu
from jax.sharding import PartitionSpec as P

LANES = 128
SCALAR_ROWS = 8
FLAG = 32.0
damping = 0.85
VMEM = pl.BlockSpec(memory_space=pltpu.VMEM)
HBM = pl.BlockSpec(memory_space=pltpu.HBM)
SMEM = pl.BlockSpec(memory_space=pltpu.SMEM)


def call(kernel, outs, scratch=(), space=VMEM, flops=1000000, scalars=(), scalar_outs=(), flags=None):
    def run(*arguments):
        return pl.pallas_call(
            kernel,
            out_shape=outs,
            in_specs=[SMEM if i in scalars else space for i in range(len(arguments))],
            out_specs=tuple(SMEM if i in scalar_outs else VMEM for i in range(len(outs))) if isinstance(outs, tuple) else VMEM,
            scratch_shapes=scratch,
            compiler_params=pltpu.CompilerParams(vmem_limit_bytes=24 * 1024 * 1024, flags=flags),
            cost_estimate=pl.CostEstimate(flops=flops, bytes_accessed=1000000, transcendentals=0),
        )(*arguments)

    return run


def prepare(*refs):
    arguments, (payload, start, dest, src, fill), (degree, dangling, sems) = refs[:6], refs[6:11], refs[11:]
    copies = [
        pltpu.make_async_copy(source, target, sems.at[i])
        for i, (source, target) in enumerate(zip(arguments, (start, degree, dangling, dest, src, fill), strict=True))
    ]
    for copy in copies:
        copy.start()
    for copy in copies:
        copy.wait()
    share = start.shape[0]
    stuck = dangling[...] > 0
    degree, rank = degree[...].astype(jnp.float32), start[...]
    scaled = (rank * (1.0 / degree)).astype(jnp.bfloat16).astype(jnp.float32)
    high = rank.astype(jnp.bfloat16).astype(jnp.float32)
    planes = [jnp.where(stuck, high, scaled), jnp.where(stuck, rank - high, degree)]
    for i, plane in enumerate(planes):
        rows = slice(i * share, (i + 1) * share)
        payload[:, rows] = jnp.broadcast_to(plane.astype(jnp.bfloat16)[None], (payload.shape[0], share, LANES))


def unpack(got, order):
    share = got.shape[1] // 2
    place = [order.index(b) for b in range(len(order))]
    one = jnp.concatenate([got[p, :share] for p in place], axis=0).astype(jnp.float32)
    two = jnp.concatenate([got[p, share:] for p in place], axis=0).astype(jnp.float32)
    return one, two, two < FLAG


def products_by_row(scaled, dest, src, fill, tiles, pages_read, sums):
    pages_read[...] = scaled.astype(jnp.bfloat16).astype(jnp.float32)
    sums[...] = jnp.zeros_like(sums)
    slots = tiles.shape[0]
    together = math.gcd(slots, 2)
    row = lax.broadcasted_iota(jnp.int32, (8, LANES), 0)
    lane = lax.broadcasted_iota(jnp.int32, (8, LANES), 1)
    for first_slot in range(0, slots, together):
        group = range(first_slot, first_slot + together)
        sources = [
            jnp.where((row == i) & (lane < fill[0, k]), pages_read[pl.ds(src[0, k], 1), :], 0.0)
            for i, k in enumerate(group)
        ]
        product = lax.dot_general(
            jnp.concatenate(sources, axis=1).astype(jnp.bfloat16),
            jnp.concatenate([tiles[k] for k in group], axis=1),
            (((1,), (1,)), ((), ())),
            preferred_element_type=jnp.float32,
        )
        for i, k in enumerate(group):
            sums[pl.ds(dest[0, k], 1), :] += product[i : i + 1]
    return sums[...]


def products_turned(scaled, dest, src, fill, turned, pages_read, dest_tiles):
    pages_read[...] = scaled.astype(jnp.bfloat16).astype(jnp.float32)
    target = lax.broadcasted_iota(jnp.int32, (dest_tiles, LANES), 0)
    lane = lax.broadcasted_iota(jnp.int32, (1, LANES), 1)
    total = jnp.zeros((dest_tiles, LANES), jnp.float32)
    slots = turned.shape[0]
    together = math.gcd(slots, 4)

    def placed(k):
        source = jnp.where(lane < fill[0, k], pages_read[pl.ds(src[0, k], 1), :], 0.0)
        return jnp.where(target == dest[0, k], source, 0.0).astype(jnp.bfloat16)

    for first_slot in range(0, slots, together):
        group = range(first_slot, first_slot + together)
        total += jnp.dot(
            jnp.concatenate([placed(k) for k in group], axis=1),
            jnp.concatenate([turned[k] for k in group], axis=0),
            preferred_element_type=jnp.float32,
        )
    return total


def first(pages, rows, order, members, got, dest, src, fill, tiles, send, pages_read, sums):
    share = got.shape[1] // 2
    one, two, stuck = unpack(got, order)
    lost = jnp.sum(jnp.where(stuck, one + two, 0.0))
    scaled = jnp.where(stuck, 0.0, one)
    total = products_by_row(scaled, dest, src, fill, tiles, pages_read, sums) + lost / pages
    for i, (_, w) in enumerate(members):
        send[i] = total[w * share : (w + 1) * share]


def gather_rows(rows, members, got, mine):
    for pair in range(mine.shape[0]):
        total = got[members.index((pair, 0))]
        for w in range(1, rows):
            total += got[members.index((pair, w))]
        mine[pair] = damping * total + (1.0 - damping)


def meanwhile(order, got, tiles, weight, flag, turned):
    _, degree, stuck = unpack(got, order)
    weight[...] = jnp.where(stuck, 0.0, 1.0 / degree)
    flag[...] = jnp.where(stuck, 1.0, 0.0)
    for k in range(tiles.shape[0]):
        turned[k] = tiles[k].T


def second(pages, rows, mine, other, weight, flag, start, dest, src, fill, turned, send, own_part, pages_read):
    share = mine.shape[1]
    b, w = lax.axis_index("blk"), lax.axis_index("row")
    core0 = lax.rem(b, 2) == 0
    pieces = []
    for pair in range(mine.shape[0]):
        pieces.append(jnp.where(core0, mine[pair], other[pair]))
        pieces.append(jnp.where(core0, other[pair], mine[pair]))
    rank = jnp.concatenate(pieces, axis=0)
    lost = jnp.sum(rank * flag[...])
    scaled = rank * weight[...]
    total = products_turned(scaled, dest, src, fill, turned, pages_read, rows * share)
    total = damping * (total + lost / pages)
    own = mine[lax.div(b, 2)]
    change = jnp.sum(jnp.abs(own - start[...]))
    own -= 1.0 - damping
    kept = jnp.zeros((share, LANES), jnp.float32)
    for r in range(rows):
        piece = total[r * share : (r + 1) * share]
        kept = jnp.where(w == r, piece, kept)
        less = jnp.where(w == r, piece - own, piece)
        for to in range(rows):
            send[to, r * share : (r + 1) * share] = less
    own_part[...] = kept
    lanes = lax.broadcasted_iota(jnp.int32, (SCALAR_ROWS, LANES), 1)
    first_lane = jnp.where(lanes == 0, change, 0.0)
    for to in range(rows):
        send[to, rows * share :] = first_lane


def block_change(got, send):
    rows, height, _ = got.shape
    dest_tiles = height - SCALAR_ROWS
    total = got[0]
    for r in range(1, rows):
        total += got[r]
    change1 = jnp.sum(jnp.abs(total[:dest_tiles]), axis=0, keepdims=True)
    both = jnp.concatenate([total[dest_tiles : dest_tiles + 1], change1], axis=0)
    send[...] = jnp.broadcast_to(both[None], (send.shape[0] // 2, 2, LANES)).reshape(send.shape)


def finish(order, got, own_part, changes, rank, out):
    share = rank.shape[0]
    w = lax.axis_index("row")
    total = own_part[...] + (1.0 - damping)
    for i, r in enumerate(order):
        total += jnp.where(w == r, 0.0, got[i, pl.ds(w * share, share), :])
    rank[...] = total
    odd = lax.rem(lax.broadcasted_iota(jnp.int32, changes.shape, 0), 2) == 1
    lane = lax.broadcasted_iota(jnp.int32, (1, LANES), 1)
    change0 = jnp.sum(jnp.where(odd, 0.0, changes[...]))
    change1 = jnp.sum(jnp.where(odd, changes[...], 0.0))
    out[...] = jnp.where(lane == 0, change0, change1)[0, : out.shape[0]]


def local(rank_start, tiles, tile_dest, tile_src, tile_fill, out_degree, dangling):
    share, slots = rank_start.shape[0], tiles.shape[0]
    blocks, rows = lax.axis_size("blk"), lax.axis_size("row")
    dest_tiles = rows * share
    by_block = list(range(blocks))[::-1]
    by_row = [*range(rows // 2, rows), *range(rows // 2)[::-1]]
    members = [(pair, w) for w in by_row for pair in range(blocks // 2)[::-1]]
    pages = float(blocks * rows * share * LANES)
    f32 = functools.partial(jax.ShapeDtypeStruct, dtype=jnp.float32)
    pages_read = (pltpu.VMEM((blocks * share, LANES), jnp.float32),)

    arguments = (rank_start, out_degree, dangling, tile_dest[None], tile_src[None], tile_fill[None])
    whole, line = (share, LANES), pltpu.SMEM((1, slots), jnp.int32)
    payload, start, *table = call(
        prepare,
        (jax.ShapeDtypeStruct((blocks, 2 * share, LANES), jnp.bfloat16), f32(whole), line, line, line),
        (pltpu.VMEM(whole, jnp.int32), pltpu.VMEM(whole, jnp.int32), pltpu.SemaphoreType.DMA((len(arguments),))),
        HBM,
        flops=1000000000,
        scalar_outs=(2, 3, 4),
    )(*(pltpu.with_memory_space_constraint(a, pltpu.HBM) for a in arguments))
    table = [pltpu.with_memory_space_constraint(a, pltpu.SMEM) for a in table]

    got_a = lax.all_to_all(payload, "blk", 0, 0, axis_index_groups=[by_block])
    send = call(
        functools.partial(first, pages, rows, by_block, members),
        f32((len(members), share, LANES)),
        (*pages_read, pltpu.VMEM((dest_tiles, LANES), jnp.float32)),
        scalars=(1, 2, 3),
    )(got_a, *table, tiles)

    groups = [[(2 * pair + core) * rows + w for pair, w in members] for core in range(2)]
    got_b = lax.all_to_all(send, ("blk", "row"), 0, 0, axis_index_groups=groups)
    mine = call(functools.partial(gather_rows, rows, members), f32((blocks // 2, share, LANES)))(got_b)
    other = lax.ppermute(mine, "blk", [(i, i ^ 1) for i in range(blocks)])
    weight, flag, turned = call(
        functools.partial(meanwhile, by_block),
        (f32((blocks * share, LANES)), f32((blocks * share, LANES)), jax.ShapeDtypeStruct(tiles.shape, tiles.dtype)),
    )(got_a, tiles)
    send, own_part = call(
        functools.partial(second, pages, rows),
        (f32((rows, dest_tiles + SCALAR_ROWS, LANES)), f32((share, LANES))),
        pages_read,
        scalars=(5, 6, 7),
    )(mine, other, weight, flag, start, *table, turned)

    got_d = lax.all_to_all(send, "row", 0, 0, axis_index_groups=[by_row])
    send = call(block_change, f32((2 * blocks, LANES)))(got_d)

    got_e = lax.all_to_all(send, "blk", 0, 0, tiled=True, axis_index_groups=[by_block])
    return call(functools.partial(finish, by_row), (f32((share, LANES)), f32((2,))))(got_d, own_part, got_e)


def solution(mesh):
    placed = (
        P(("blk", "row"), None),
        P(("blk", "row"), None, None),
        P(("blk", "row")),
        P(("blk", "row")),
        P(("blk", "row")),
        P(("blk", "row"), None),
        P(("blk", "row"), None),
    )
    return jax.shard_map(
        local, mesh=mesh, in_specs=placed, out_specs=(P(("blk", "row"), None), P()), check_vma=False
    )
```

```python
import functools
import math

import jax
import jax.numpy as jnp
from jax import lax
from jax.experimental import pallas as pl
from jax.experimental.pallas import tpu as pltpu
from jax.sharding import PartitionSpec as P

LANES = 128
SCALAR_ROWS = 8
FLAG = 32.0
damping = 0.85
VMEM = pl.BlockSpec(memory_space=pltpu.VMEM)
HBM = pl.BlockSpec(memory_space=pltpu.HBM)
SMEM = pl.BlockSpec(memory_space=pltpu.SMEM)


def call(kernel, outs, scratch=(), space=VMEM, flops=1000000, scalars=(), scalar_outs=(), flags=None):
    def run(*arguments):
        return pl.pallas_call(
            kernel,
            out_shape=outs,
            in_specs=[SMEM if i in scalars else space for i in range(len(arguments))],
            out_specs=tuple(SMEM if i in scalar_outs else VMEM for i in range(len(outs))) if isinstance(outs, tuple) else VMEM,
            scratch_shapes=scratch,
            compiler_params=pltpu.CompilerParams(vmem_limit_bytes=24 * 1024 * 1024, flags=flags),
            cost_estimate=pl.CostEstimate(flops=flops, bytes_accessed=1000000, transcendentals=0),
        )(*arguments)

    return run


def prepare(*refs):
    arguments, (payload, start, dest, src, fill), (degree, dangling, sems) = refs[:6], refs[6:11], refs[11:]
    copies = [
        pltpu.make_async_copy(source, target, sems.at[i])
        for i, (source, target) in enumerate(zip(arguments, (start, degree, dangling, dest, src, fill), strict=True))
    ]
    for copy in copies:
        copy.start()
    for copy in copies:
        copy.wait()
    share = start.shape[0]
    stuck = dangling[...] > 0
    degree, rank = degree[...].astype(jnp.float32), start[...]
    scaled = (rank * (1.0 / degree)).astype(jnp.bfloat16).astype(jnp.float32)
    high = rank.astype(jnp.bfloat16).astype(jnp.float32)
    planes = [jnp.where(stuck, high, scaled), jnp.where(stuck, rank - high, degree)]
    for i, plane in enumerate(planes):
        rows = slice(i * share, (i + 1) * share)
        payload[:, rows] = jnp.broadcast_to(plane.astype(jnp.bfloat16)[None], (payload.shape[0], share, LANES))


def unpack(got, order):
    share = got.shape[1] // 2
    place = [order.index(b) for b in range(len(order))]
    one = jnp.concatenate([got[p, :share] for p in place], axis=0).astype(jnp.float32)
    two = jnp.concatenate([got[p, share:] for p in place], axis=0).astype(jnp.float32)
    return one, two, two < FLAG


def products_by_row(scaled, dest, src, fill, tiles, pages_read, sums):
    pages_read[...] = scaled.astype(jnp.bfloat16).astype(jnp.float32)
    sums[...] = jnp.zeros_like(sums)
    slots = tiles.shape[0]
    together = math.gcd(slots, 2)
    row = lax.broadcasted_iota(jnp.int32, (8, LANES), 0)
    lane = lax.broadcasted_iota(jnp.int32, (8, LANES), 1)
    for first_slot in range(0, slots, together):
        group = range(first_slot, first_slot + together)
        sources = [
            jnp.where((row == i) & (lane < fill[0, k]), pages_read[pl.ds(src[0, k], 1), :], 0.0)
            for i, k in enumerate(group)
        ]
        product = lax.dot_general(
            jnp.concatenate(sources, axis=1).astype(jnp.bfloat16),
            jnp.concatenate([tiles[k] for k in group], axis=1),
            (((1,), (1,)), ((), ())),
            preferred_element_type=jnp.float32,
        )
        for i, k in enumerate(group):
            sums[pl.ds(dest[0, k], 1), :] += product[i : i + 1]
    return sums[...]


def products_turned(scaled, dest, src, fill, turned, pages_read, dest_tiles):
    pages_read[...] = scaled.astype(jnp.bfloat16).astype(jnp.float32)
    target = lax.broadcasted_iota(jnp.int32, (dest_tiles, LANES), 0)
    lane = lax.broadcasted_iota(jnp.int32, (1, LANES), 1)
    total = jnp.zeros((dest_tiles, LANES), jnp.float32)
    slots = turned.shape[0]
    together = math.gcd(slots, 4)

    def placed(k):
        source = jnp.where(lane < fill[0, k], pages_read[pl.ds(src[0, k], 1), :], 0.0)
        return jnp.where(target == dest[0, k], source, 0.0).astype(jnp.bfloat16)

    for first_slot in range(0, slots, together):
        group = range(first_slot, first_slot + together)
        total += jnp.dot(
            jnp.concatenate([placed(k) for k in group], axis=1),
            jnp.concatenate([turned[k] for k in group], axis=0),
            preferred_element_type=jnp.float32,
        )
    return total


def first(pages, rows, order, members, got, dest, src, fill, tiles, send, pages_read, sums):
    share = got.shape[1] // 2
    one, two, stuck = unpack(got, order)
    lost = jnp.sum(jnp.where(stuck, one + two, 0.0))
    scaled = jnp.where(stuck, 0.0, one)
    total = products_by_row(scaled, dest, src, fill, tiles, pages_read, sums) + lost / pages
    for i, (_, w) in enumerate(members):
        send[i] = total[w * share : (w + 1) * share]


def gather_rows(rows, members, got, mine):
    for pair in range(mine.shape[0]):
        total = got[members.index((pair, 0))]
        for w in range(1, rows):
            total += got[members.index((pair, w))]
        mine[pair] = damping * total + (1.0 - damping)


def meanwhile(order, got, tiles, weight, flag, turned):
    _, degree, stuck = unpack(got, order)
    weight[...] = jnp.where(stuck, 0.0, 1.0 / degree)
    flag[...] = jnp.where(stuck, 1.0, 0.0)
    for k in range(tiles.shape[0]):
        turned[k] = tiles[k].T


def second(pages, rows, mine, other, weight, flag, start, dest, src, fill, turned, send, own_part, pages_read):
    share = mine.shape[1]
    b, w = lax.axis_index("blk"), lax.axis_index("row")
    core0 = lax.rem(b, 2) == 0
    pieces = []
    for pair in range(mine.shape[0]):
        pieces.append(jnp.where(core0, mine[pair], other[pair]))
        pieces.append(jnp.where(core0, other[pair], mine[pair]))
    rank = jnp.concatenate(pieces, axis=0)
    lost = jnp.sum(rank * flag[...])
    scaled = rank * weight[...]
    total = products_turned(scaled, dest, src, fill, turned, pages_read, rows * share)
    total = damping * (total + lost / pages)
    own = mine[lax.div(b, 2)]
    change = jnp.sum(jnp.abs(own - start[...]), axis=0, keepdims=True)
    own -= 1.0 - damping
    kept = jnp.zeros((share, LANES), jnp.float32)
    for r in range(rows):
        piece = total[r * share : (r + 1) * share]
        kept = jnp.where(w == r, piece, kept)
        less = jnp.where(w == r, piece - own, piece)
        for to in range(rows):
            send[to, r * share : (r + 1) * share] = less
    own_part[...] = kept
    for to in range(rows):
        send[to, rows * share :] = jnp.broadcast_to(change, (SCALAR_ROWS, LANES))


def block_change(got, send):
    rows, height, _ = got.shape
    dest_tiles = height - SCALAR_ROWS
    total = got[0]
    for r in range(1, rows):
        total += got[r]
    change1 = jnp.sum(jnp.abs(total[:dest_tiles]), axis=0, keepdims=True)
    both = jnp.concatenate([total[dest_tiles : dest_tiles + 1], change1], axis=0)
    send[...] = jnp.broadcast_to(both[None], (send.shape[0] // 2, 2, LANES)).reshape(send.shape)


def finish(order, got, own_part, changes, rank, out):
    share = rank.shape[0]
    w = lax.axis_index("row")
    total = own_part[...] + (1.0 - damping)
    for i, r in enumerate(order):
        total += jnp.where(w == r, 0.0, got[i, pl.ds(w * share, share), :])
    rank[...] = total
    odd = lax.rem(lax.broadcasted_iota(jnp.int32, changes.shape, 0), 2) == 1
    lane = lax.broadcasted_iota(jnp.int32, (1, LANES), 1)
    change0 = jnp.sum(jnp.where(odd, 0.0, changes[...]))
    change1 = jnp.sum(jnp.where(odd, changes[...], 0.0))
    out[...] = jnp.where(lane == 0, change0, change1)[0, : out.shape[0]]


def local(rank_start, tiles, tile_dest, tile_src, tile_fill, out_degree, dangling):
    share, slots = rank_start.shape[0], tiles.shape[0]
    blocks, rows = lax.axis_size("blk"), lax.axis_size("row")
    dest_tiles = rows * share
    by_block = list(range(blocks))[::-1]
    by_row = [*range(rows // 2, rows), *range(rows // 2)[::-1]]
    members = [(pair, w) for w in by_row for pair in range(blocks // 2)[::-1]]
    pages = float(blocks * rows * share * LANES)
    f32 = functools.partial(jax.ShapeDtypeStruct, dtype=jnp.float32)
    pages_read = (pltpu.VMEM((blocks * share, LANES), jnp.float32),)

    arguments = (rank_start, out_degree, dangling, tile_dest[None], tile_src[None], tile_fill[None])
    whole, line = (share, LANES), pltpu.SMEM((1, slots), jnp.int32)
    payload, start, *table = call(
        prepare,
        (jax.ShapeDtypeStruct((blocks, 2 * share, LANES), jnp.bfloat16), f32(whole), line, line, line),
        (pltpu.VMEM(whole, jnp.int32), pltpu.VMEM(whole, jnp.int32), pltpu.SemaphoreType.DMA((len(arguments),))),
        HBM,
        flops=1000000000,
        scalar_outs=(2, 3, 4),
    )(*(pltpu.with_memory_space_constraint(a, pltpu.HBM) for a in arguments))
    table = [pltpu.with_memory_space_constraint(a, pltpu.SMEM) for a in table]

    got_a = lax.all_to_all(payload, "blk", 0, 0, axis_index_groups=[by_block])
    send = call(
        functools.partial(first, pages, rows, by_block, members),
        f32((len(members), share, LANES)),
        (*pages_read, pltpu.VMEM((dest_tiles, LANES), jnp.float32)),
        scalars=(1, 2, 3),
    )(got_a, *table, tiles)

    groups = [[(2 * pair + core) * rows + w for pair, w in members] for core in range(2)]
    got_b = lax.all_to_all(send, ("blk", "row"), 0, 0, axis_index_groups=groups)
    mine = call(functools.partial(gather_rows, rows, members), f32((blocks // 2, share, LANES)))(got_b)
    other = lax.ppermute(mine, "blk", [(i, i ^ 1) for i in range(blocks)])
    weight, flag, turned = call(
        functools.partial(meanwhile, by_block),
        (f32((blocks * share, LANES)), f32((blocks * share, LANES)), jax.ShapeDtypeStruct(tiles.shape, tiles.dtype)),
    )(got_a, tiles)
    send, own_part = call(
        functools.partial(second, pages, rows),
        (f32((rows, dest_tiles + SCALAR_ROWS, LANES)), f32((share, LANES))),
        pages_read,
        scalars=(5, 6, 7),
    )(mine, other, weight, flag, start, *table, turned)

    got_d = lax.all_to_all(send, "row", 0, 0, axis_index_groups=[by_row])
    send = call(block_change, f32((2 * blocks, LANES)))(got_d)

    got_e = lax.all_to_all(send, "blk", 0, 0, tiled=True, axis_index_groups=[by_block])
    return call(functools.partial(finish, by_row), (f32((share, LANES)), f32((2,))))(got_d, own_part, got_e)


def solution(mesh):
    placed = (
        P(("blk", "row"), None),
        P(("blk", "row"), None, None),
        P(("blk", "row")),
        P(("blk", "row")),
        P(("blk", "row")),
        P(("blk", "row"), None),
        P(("blk", "row"), None),
    )
    return jax.shard_map(
        local, mesh=mesh, in_specs=placed, out_specs=(P(("blk", "row"), None), P()), check_vma=False
    )
```
